32 devices in a mesh: sub: 32 (over z, y, x, core).
Axes of the slice: x: 2, y: 2, z: 4, core: 2. Of those that a mesh axis runs over, the one named last changes fastest.
Arguments:
- right_side: float32 [128, 128, 512], P('sub'), may hold values from -8 to 8
- sigma: float32 [128, 128, 512], P('sub'), may hold values from 0.25 to 2
- wind: float32 [128, 128, 512], P('sub'), may hold values from -0.8 to 0.8
- local_inverse: float32 [32, 512, 512], P('sub'), may hold values from -1 to 2, as said below
- basis_y: float32 [128, 32], replicated, may hold values from -0.5 to 0.5
- basis_z: float32 [512, 64], replicated, may hold values from -0.25 to 0.25
- gamma: float32 [5, 32, 64], replicated, may hold values from 0.3 to 3
Outputs:
- solution_field: float32 [128, 128, 512], P('sub')
- residual: float32 [128, 128, 512], P('sub')
The draws below stay inside these ranges and needn't reach their ends.
Inputs may be any that keep to these rules, and one draw needn't show every extreme that they name: `local_inverse`: each block is the identity plus a perturbation whose entries lie within 2/sqrt(512) of zero; each row of the perturbation has norm about one half.
All inputs are finite; a program needn't handle non-finite values.
Results may differ from the reference program's by a relative error of at most 0.00022.
Values sent between devices are 32-bit elements; how exact they have to be, the bound alone decides.
A program may use at most 64 MiB of HBM per device.

```python
import math
import jax
import jax.numpy as jnp
from jax import lax

CX = 4
NY = 128
NZ = 512
KY = 32
KZ = 64
BLOCKS = 32
NX = 128
LEVELS = 5
N_SUB = 32


def draw_local_inverse(key, part):
    noise = jnp.clip(jax.random.normal(key, (BLOCKS, NZ, NZ), jnp.float32), -4.0, 4.0)
    scaled = noise * (0.5 / jnp.sqrt(jnp.float32(NZ)))
    return scaled + jnp.eye(NZ, dtype=jnp.float32)[None]


def block_scale(own_key, shape, split, low, top_value):
    def one(axis_at, shards_of):
        steps = jax.random.uniform(jax.random.fold_in(jax.random.fold_in(own_key, 6), axis_at), (shards_of,), jnp.float32, low / len(split), top_value / len(split))
        return jnp.repeat(jnp.exp(steps), shape[axis_at] // shards_of).reshape((-1,) + (1,) * (len(shape) - axis_at - 1))

    gain = one(*split[0])
    for cut in split[1:]:
        gain = gain * one(*cut)
    return gain


def bell_draw(key, extent, deviation, reach, pieces=(), held_as=jnp.bfloat16):
    loudness = block_scale(key, extent, pieces, -0.22, 0.18) if pieces else 1.0
    result = jax.random.normal(key, extent, jnp.float32) * deviation * loudness
    return jnp.minimum(jnp.maximum(result, -reach), reach).astype(held_as)


def setup_inputs(seed: int = 0) -> dict:
    key_list = jax.random.split(jax.random.key(seed), 8)
    return {
        "right_side": bell_draw(key_list[0], (NX, NY, NZ), 1.0, 8.0, ((0, 32),), jnp.float32),
        "sigma": jnp.clip(0.25 + 1.75 * jax.random.uniform(key_list[1], (NX, NY, NZ), jnp.float32) ** block_scale(key_list[1], (NX, NY, NZ), ((0, 32),), -0.2, 0.2), 0.25, 2.0),
        "wind": jnp.clip(jax.random.uniform(key_list[2], (NX, NY, NZ), jnp.float32, -0.8, 0.8) * block_scale(key_list[2], (NX, NY, NZ), ((0, 32),), -0.4, 0.0), -0.8, 0.8),
        "local_inverse": draw_local_inverse(jax.random.fold_in(key_list[7], 71), 0),
        "basis_y": bell_draw(key_list[4], (NY, KY), NY ** -0.5, 0.5, (), jnp.float32),
        "basis_z": bell_draw(key_list[5], (NZ, KZ), NZ ** -0.5, 0.25, (), jnp.float32),
        "gamma": jnp.clip(jnp.exp(jax.random.uniform(key_list[6], (LEVELS, KY, KZ), jnp.float32, math.log(0.3), math.log(3.0))), 0.3, 3.0),
    }


HIGH = lax.Precision.HIGHEST

def apply_operator(field, sigma, wind):
    padded_x = jnp.pad(field, ((1, 1), (0, 0), (0, 0)))
    upper = padded_x[2:]
    lower = padded_x[:-2]
    padded_y = jnp.pad(field, ((0, 0), (1, 1), (0, 0)))
    padded_z = jnp.pad(field, ((0, 0), (0, 0), (1, 1)))
    beside = upper + lower + padded_y[:, 2:] + padded_y[:, :-2] + padded_z[:, :, 2:] + padded_z[:, :, :-2]
    return (6.0 + sigma) * field - beside + wind * (upper - lower)

def precondition(field, local_inverse, basis_y, basis_z, gamma):
    blocks = field.reshape(N_SUB, CX, NY, NZ)
    local = jnp.einsum('bxyz,bzw->bxyw', blocks, local_inverse, precision=HIGH)
    summed = lax.optimization_barrier(jnp.sum(blocks, axis=1))
    half = jnp.einsum('byz,zm->bym', summed, basis_z, precision=HIGH)
    proj = jnp.einsum('yk,bym->bkm', basis_y, half, precision=HIGH)
    coarse = jnp.zeros((N_SUB, KY, KZ), jnp.float32)
    for level in range(LEVELS):
        width = 2 ** (level + 1)
        grouped = lax.optimization_barrier(jnp.sum(proj.reshape(N_SUB // width, width, KY, KZ), axis=1, keepdims=True))
        grouped = jnp.broadcast_to(grouped, (N_SUB // width, width, KY, KZ)).reshape(N_SUB, KY, KZ)
        coarse = coarse + gamma[level] * grouped / jnp.sqrt(jnp.float32(CX * width))
    back = jnp.einsum('bkm,zm->bkz', coarse, basis_z, precision=HIGH)
    spread = jnp.einsum('yk,bkz->byz', basis_y, back, precision=HIGH)
    return (local + spread[:, None]).reshape(NX, NY, NZ)

def reference(right_side, sigma, wind, local_inverse, basis_y, basis_z, gamma):

    def inner(left, right):
        return jnp.sum(left * right)
    beta = jnp.sqrt(inner(right_side, right_side))
    first = right_side / beta
    z_one = precondition(first, local_inverse, basis_y, basis_z, gamma)
    image = apply_operator(z_one, sigma, wind)
    h11 = inner(first, image)
    image = image - h11 * first
    h21 = jnp.sqrt(inner(image, image))
    second = image / h21
    z_two = precondition(second, local_inverse, basis_y, basis_z, gamma)
    image = apply_operator(z_two, sigma, wind)
    h12 = inner(first, image)
    h22 = inner(second, image)
    image = image - h12 * first - h22 * second
    h32 = jnp.sqrt(inner(image, image))
    m11 = h11 * h11 + h21 * h21
    m12 = h11 * h12 + h21 * h22
    m22 = h12 * h12 + h22 * h22 + h32 * h32
    q_one = h11 * beta
    q_two = h12 * beta
    determ = m11 * m22 - m12 * m12
    y_one = (m22 * q_one - m12 * q_two) / determ
    y_two = (m11 * q_two - m12 * q_one) / determ
    solution_field = y_one * z_one + y_two * z_two
    residual = right_side - apply_operator(solution_field, sigma, wind)
    return (solution_field, residual)
```

```python
import functools

import jax
import jax.numpy as jnp
from jax import lax
from jax.experimental import pallas as pl
from jax.experimental.pallas import tpu as pltpu
from jax.sharding import PartitionSpec as P

HIGH = lax.Precision.HIGHEST
MESH = pl.DeviceIdType.MESH
PAD = 8


def split(x):
    hi = x.astype(jnp.bfloat16)
    lo = (x - hi.astype(jnp.float32)).astype(jnp.bfloat16)
    return hi, lo


def mm(a, b):
    return jnp.dot(a, b, preferred_element_type=jnp.float32)


def mt(a, b):
    return lax.dot_general(
        a, b, (((1,), (1,)), ((), ())), preferred_element_type=jnp.float32
    )


def tm(a, b):
    return lax.dot_general(
        a, b, (((0,), (0,)), ((), ())), preferred_element_type=jnp.float32
    )


def fold(x):
    part = jnp.sum(x, axis=0, keepdims=True)
    out = part[:, 0:128]
    for at in range(128, part.shape[1], 128):
        out = out + part[:, at : at + 128]
    return out


def flip(i, mask):
    out, bit = i, 1
    while bit <= mask:
        if mask & bit:
            out = out + bit - 2 * bit * lax.rem(lax.div(i, bit), 2)
        bit *= 2
    return out


def drain(ref, sem):
    pltpu.make_async_copy(ref, ref, sem).wait()


def kernel(
    n, block,
    r_hbm, sg_hbm, wd_hbm, li_hbm, by_hbm, bz_hbm, gm_hbm,
    r, u1, u2, w1, w2, coef,
    sg, wd, lf, by, bz, gm, lh, ll, by3, bz3, hs, hr,
    own, gat, tot, allb, low_s, low_r, nbr, gs, ggat,
    in_sem, sa, ra, sb, rb, se, re, sh, rh, sga, rga,
):
    layers, rows, depth = r.shape
    ky = by.shape[0]
    half = ky // 2
    kz = bz.shape[0]
    levels = gm.shape[0]
    blocks = n // block
    low_levels = block.bit_length() - 1
    me = lax.axis_index("sub")
    p = lax.rem(me, block)
    z = lax.div(me, block)
    us = (u1, u2)
    ws = (w1, w2)

    def load(i, src, dst):
        c = pltpu.make_async_copy(src, dst, in_sem.at[i])
        c.start()
        return c

    c_r = load(0, r_hbm, r)
    c_bz = load(1, bz_hbm, bz)
    c_by = load(2, by_hbm, by)
    c_l = load(3, li_hbm, lf)
    c_gm = load(4, gm_hbm, gm)

    barrier = pltpu.get_barrier_semaphore()
    in_block = [z * block + flip(p, d) for d in range(block - 1, 0, -1)]
    across = [lax.rem(z + d, blocks) * block + p for d in range(1, blocks)]
    first_cross = jnp.logical_and(p == 0, z > 0)
    last_cross = jnp.logical_and(p == block - 1, z < blocks - 1)

    def signal(target):
        pl.semaphore_signal(barrier, inc=1, device_id=(target,), device_id_type=MESH)

    for target in in_block + across:
        signal(target)

    @pl.when(first_cross)
    def _():
        signal(me - 1)

    @pl.when(last_cross)
    def _():
        signal(me + 1)

    zero_rows = jnp.zeros((PAD, depth), jnp.float32)
    for u in us:
        for l in range(1, layers + 1):
            u[l, 0:PAD, :] = zero_rows
            u[l, PAD + rows : PAD + rows + PAD, :] = zero_rows

    def send(src, dst, s, q, target):
        return pltpu.make_async_remote_copy(
            src_ref=src, dst_ref=dst, send_sem=s, recv_sem=q,
            device_id=(target,), device_id_type=MESH,
        )

    def project(k, field):
        summed = field[0]
        for l in range(1, layers):
            summed = summed + field[l]
        sh_, sl_ = split(summed)
        bh, bl = bz3[0:kz], bz3[2 * kz : 3 * kz]
        part = mt(sh_, bh) + mt(sl_, bh) + mt(sh_, bl)
        ph, pl_ = split(part)
        bh, bl = by3[0:ky], by3[2 * ky : 3 * ky]
        full = mm(bh, ph) + mm(bh, pl_) + mm(bl, ph)
        packed = jnp.concatenate([full[0:half], full[half:ky]], axis=1)
        own[k] = packed
        gat[k, p] = packed

    def a_send(k):
        for target in in_block:
            send(own.at[k], gat.at[k, p], sa.at[k], ra.at[k], target).start()

    def a_wait(k, sem):
        drain(gat.at[k, pl.ds(0, block - 1)], sem.at[k])

    def b_send(k):
        for target in across:
            send(tot.at[k], allb.at[k, z], sb.at[k], rb.at[k], target).start()

    def b_wait(k, sem):
        if blocks > 1:
            drain(allb.at[k, pl.ds(0, blocks - 1)], sem.at[k])

    def down(k):
        return send(hs.at[k, 0], hr.at[k, 1], sh.at[k, 0], rh.at[k, 1], me - 1)

    def up(k):
        return send(hs.at[k, 1], hr.at[k, 0], sh.at[k, 1], rh.at[k, 0], me + 1)

    def low_down(k):
        return send(low_s.at[k, 0], low_r.at[k, 1], se.at[k, 0], re.at[k, 1], me - block)

    def low_up(k):
        return send(low_s.at[k, 1], low_r.at[k, 0], se.at[k, 1], re.at[k, 0], me + block)

    def local(x):
        xh, xl = split(x)
        return mm(xh, lh[...]) + mm(xl, lh[...]) + mm(xh, ll[...])

    def factor(level):
        g = gm[level]
        return jnp.concatenate([g[0:half], g[half:ky]], axis=1) * (
            (layers * 2 ** (level + 1)) ** -0.5
        )

    def low_part(k, q, upper):
        out = None
        for level in range(low_levels):
            width = 2 ** (level + 1)
            start = lax.div(q, width) * width
            if width == block:
                acc = tot[k]
            else:
                acc = gat[k, start]
                for j in range(1, width):
                    acc = acc + gat[k, start + j]
            term = upper[level] * acc
            out = term if out is None else out + term
        return out

    def high_part(k, zz, upper):
        out = jnp.zeros(tot.shape[1:], jnp.float32)
        for level in range(low_levels, levels):
            width = 2 ** (level + 1) // block
            start = lax.div(zz, width) * width
            acc = allb[k, start]
            for j in range(1, width):
                acc = acc + allb[k, start + j]
            out = out + upper[level] * acc
        return out

    def edges(k, field):
        first = local(field[0])
        hs[k, 0] = first

        @pl.when(me > 0)
        def _():
            down(k).start()

        us[k][1, PAD : PAD + rows, :] = first
        last = local(field[layers - 1])
        hs[k, 1] = last

        @pl.when(me < n - 1)
        def _():
            up(k).start()

        us[k][layers, PAD : PAD + rows, :] = last

    def middle(k, field):
        for l in range(1, layers - 1):
            us[k][l + 1, PAD : PAD + rows, :] = local(field[l])

    def exchange(k):
        fac = [factor(level) for level in range(levels)]
        a_wait(k, ra)
        acc = gat[k, 0]
        for j in range(1, block):
            acc = acc + gat[k, j]
        tot[k] = acc
        allb[k, z] = acc
        b_send(k)

        @pl.when(jnp.logical_and(p == block - 1, z > 0))
        def _():
            low_s[k, 0] = low_part(k, 0, fac)
            low_down(k).start()

        @pl.when(jnp.logical_and(p == 0, z < blocks - 1))
        def _():
            low_s[k, 1] = low_part(k, block - 1, fac)
            low_up(k).start()

        nbr[1] = low_part(k, p, fac)

        @pl.when(p > 0)
        def _():
            nbr[0] = low_part(k, p - 1, fac)

        @pl.when(p < block - 1)
        def _():
            nbr[2] = low_part(k, p + 1, fac)

        @pl.when(jnp.logical_and(p == 0, z == 0))
        def _():
            nbr[0] = jnp.zeros(nbr.shape[1:], jnp.float32)

        @pl.when(jnp.logical_and(p == block - 1, z == blocks - 1))
        def _():
            nbr[2] = jnp.zeros(nbr.shape[1:], jnp.float32)

        b_wait(k, rb)

        @pl.when(first_cross)
        def _():
            low_up(k).wait_recv()
            nbr[0] = low_r[k, 0]

        @pl.when(last_cross)
        def _():
            low_down(k).wait_recv()
            nbr[2] = low_r[k, 1]

        here = high_part(k, z, fac)
        before = high_part(k, lax.div(lax.rem(me + n - 1, n), block), fac)
        after = high_part(k, lax.div(lax.rem(me + 1, n), block), fac)
        three = []
        for c in (nbr[0] + before, nbr[1] + here, nbr[2] + after):
            three += [c[:, 0:kz], c[:, kz : 2 * kz]]
        stack = jnp.concatenate(three, axis=0)
        th, tl = split(stack)
        back = mm(jnp.concatenate([th, tl, th], axis=1), bz3[...])
        th, tl = split(back)
        spreads = []
        for j in range(3):
            piece = slice(j * ky, (j + 1) * ky)
            spreads.append(
                tm(by3[...], jnp.concatenate([th[piece], tl[piece], th[piece]], axis=0))
            )
        u = us[k]
        mine = spreads[1]
        for l in range(1, layers + 1):
            u[l, PAD : PAD + rows, :] = u[l, PAD : PAD + rows, :] + mine
        u[0, PAD : PAD + rows, :] = jnp.where(me > 0, spreads[0], 0.0)
        u[layers + 1, PAD : PAD + rows, :] = jnp.where(me < n - 1, spreads[2], 0.0)

    step = 32

    def operator(k, l):
        u = us[k]
        col = lax.broadcasted_iota(jnp.int32, (step, depth), 1)
        for y in range(0, rows, step):
            a = PAD + y
            c = u[l + 1, a : a + step, :]
            hi = u[l + 2, a : a + step, :]
            lo = u[l, a : a + step, :]
            fwd = jnp.where(col == depth - 1, 0.0, pltpu.roll(c, depth - 1, 1))
            bwd = jnp.where(col == 0, 0.0, pltpu.roll(c, 1, 1))
            beside = (
                hi + lo + u[l + 1, a + 1 : a + step + 1, :]
                + u[l + 1, a - 1 : a + step - 1, :] + fwd + bwd
            )
            ws[k][l, y : y + step, :] = (
                (6.0 + sg[l, y : y + step, :]) * c - beside
                + wd[l, y : y + step, :] * (hi - lo)
            )

    def stencil(k):
        for l in range(layers):
            operator(k, l)

    def meet(k):
        w = ws[k]

        @pl.when(me > 0)
        def _():
            up(k).wait_recv()
            w[0] = w[0] - (1.0 + wd[0]) * hr[k, 0]

        @pl.when(me < n - 1)
        def _():
            down(k).wait_recv()
            w[layers - 1] = w[layers - 1] + (wd[layers - 1] - 1.0) * hr[k, 1]

    def dots(pairs, which):
        out = []
        for a, b in pairs:
            acc = None
            for l in which:
                term = a[l] * b[l]
                acc = term if acc is None else acc + term
            out.append(fold(acc))
        return out

    def triple(src, dst):
        hi, lo = split(src[...])
        m = src.shape[0]
        dst[0:m] = hi
        dst[m : 2 * m] = hi
        dst[2 * m : 3 * m] = lo

    c_bz.wait()
    triple(bz, bz3)
    c_by.wait()
    triple(by, by3)
    c_r.wait()
    project(0, r)
    extra = jnp.where(first_cross, 1, 0) + jnp.where(last_cross, 1, 0)
    pl.semaphore_wait(barrier, block - 1 + blocks - 1 + extra)
    a_send(0)
    c_l.wait()
    c_sg = load(5, sg_hbm, sg)
    c_wd = load(6, wd_hbm, wd)
    big, small = split(lf[0])
    lh[...] = big
    ll[...] = small
    edges(0, r)
    middle(0, r)
    c_gm.wait()
    exchange(0)
    c_sg.wait()
    c_wd.wait()
    stencil(0)
    meet(0)

    project(1, w1)
    a_send(1)
    edges(1, w1)
    middle(1, w1)
    early = dots([(r, r), (r, w1), (w1, w1)], range(layers))
    exchange(1)
    stencil(1)
    pairs = [(r, w2), (w1, w2), (w2, w2)]
    inside = dots(pairs, range(1, layers - 1))
    meet(1)
    late = [i + o for i, o in zip(inside, dots(pairs, (0, layers - 1)))]
    blank = jnp.zeros((2, 128), jnp.float32)
    sums = jnp.sum(jnp.concatenate(early + late + [blank], axis=0), axis=1, keepdims=True)
    row = lax.broadcasted_iota(jnp.int32, (8, 128), 0)
    lane = lax.broadcasted_iota(jnp.int32, (8, 128), 1)
    flat = jnp.sum(jnp.where(row == lane, sums, 0.0), axis=0, keepdims=True)
    gs[...] = flat
    ggat[me] = flat

    for d in range(n - 1, 0, -1):
        send(gs, ggat.at[me], sga, rga, flip(me, d)).start()
    drain(ggat.at[pl.ds(0, n - 1)], rga)
    total = jnp.sum(ggat[...], axis=0)
    g01, g11, g02, g12, g22 = (total[:, j : j + 1] for j in range(1, 6))
    ratio = g12 / g11
    c2 = (g02 - ratio * g01) / (g22 - ratio * g12)
    c1 = g01 / g11 - ratio * c2
    coef[0:1, :] = jnp.broadcast_to(c1, (1, 128))
    coef[1:2, :] = jnp.broadcast_to(c2, (1, 128))

    for k in range(2):
        a_wait(k, sa)
        b_wait(k, sb)

        @pl.when(jnp.logical_and(p == block - 1, z > 0))
        def _():
            low_down(k).wait_send()

        @pl.when(jnp.logical_and(p == 0, z < blocks - 1))
        def _():
            low_up(k).wait_send()

        @pl.when(me > 0)
        def _():
            down(k).wait_send()

        @pl.when(me < n - 1)
        def _():
            up(k).wait_send()

    drain(ggat.at[pl.ds(0, n - 1)], sga)


def finish(r, u1, u2, w1, w2, coef, x_hbm, res_hbm, xo, ro, out_sem, res_sem):
    layers, rows, depth = r.shape
    step = 32
    c1 = coef[0:1, 0:1]
    c2 = coef[1:2, 0:1]
    for l in range(layers):
        for y in range(0, rows, step):
            a = PAD + y
            xo[l, y : y + step, :] = (
                c1 * u1[l + 1, a : a + step, :] + c2 * u2[l + 1, a : a + step, :]
            )
        pltpu.make_async_copy(xo.at[l], x_hbm.at[l], out_sem).start()
    for l in range(layers):
        for y in range(0, rows, step):
            ro[l, y : y + step, :] = (
                r[l, y : y + step, :]
                - c1 * w1[l, y : y + step, :] - c2 * w2[l, y : y + step, :]
            )
        pltpu.make_async_copy(ro.at[l], res_hbm.at[l], res_sem).start()
    drain(xo, out_sem)
    drain(ro, res_sem)


def on_device(right_side, sigma, wind, local_inverse, basis_y, basis_z, gamma):
    n = lax.axis_size("sub")
    block = min(8, n)
    blocks = n // block
    layers, rows, depth = right_side.shape
    ky = basis_y.shape[1]
    kz = basis_z.shape[1]
    levels = gamma.shape[0]
    f32 = jnp.float32
    packed = (ky // 2, 2 * kz)
    cube = pltpu.VMEM((layers, rows, depth), f32)
    padded = pltpu.VMEM((layers + 2, rows + 2 * PAD, depth), f32)
    dma = pltpu.SemaphoreType.DMA
    scratch = [
        cube, cube,
        pltpu.VMEM((1, depth, depth), f32),
        pltpu.VMEM((ky, rows), f32),
        pltpu.VMEM((kz, depth), f32),
        pltpu.VMEM(gamma.shape, f32),
        pltpu.VMEM((depth, depth), jnp.bfloat16),
        pltpu.VMEM((depth, depth), jnp.bfloat16),
        pltpu.VMEM((3 * ky, rows), jnp.bfloat16),
        pltpu.VMEM((3 * kz, depth), jnp.bfloat16),
        pltpu.VMEM((2, 2, rows, depth), f32),
        pltpu.VMEM((2, 2, rows, depth), f32),
        pltpu.VMEM((2,) + packed, f32),
        pltpu.VMEM((2, block) + packed, f32),
        pltpu.VMEM((2,) + packed, f32),
        pltpu.VMEM((2, blocks) + packed, f32),
        pltpu.VMEM((2, 2) + packed, f32),
        pltpu.VMEM((2, 2) + packed, f32),
        pltpu.VMEM((3,) + packed, f32),
        pltpu.VMEM((1, 128), f32),
        pltpu.VMEM((n, 1, 128), f32),
        dma((7,)),
        dma((2,)), dma((2,)),
        dma((2,)), dma((2,)),
        dma((2, 2)), dma((2, 2)),
        dma((2, 2)), dma((2, 2)),
        dma, dma,
    ]
    hbm = pl.BlockSpec(memory_space=pltpu.HBM)
    vmem = pl.BlockSpec(memory_space=pltpu.VMEM)
    out = jax.ShapeDtypeStruct(right_side.shape, f32)
    pieces = pl.pallas_call(
        functools.partial(kernel, n, block),
        out_shape=(cube, padded, padded, cube, cube, pltpu.VMEM((8, 128), f32)),
        in_specs=[hbm] * 7,
        out_specs=(vmem,) * 6,
        scratch_shapes=scratch,
        compiler_params=pltpu.CompilerParams(
            collective_id=0, has_side_effects=True, vmem_limit_bytes=50 * 2**20,
        ),
        name="gmres",
    )(right_side, sigma, wind, local_inverse, basis_y.T, basis_z.T, gamma)
    return pl.pallas_call(
        finish,
        out_shape=(out, out),
        in_specs=[vmem] * 6,
        out_specs=(hbm, hbm),
        scratch_shapes=[cube, cube, dma, dma],
        compiler_params=pltpu.CompilerParams(vmem_limit_bytes=24 * 2**20),
        name="finish",
    )(*pieces)


def solution(mesh):
    placed = (
        P("sub", None, None),
        P("sub", None, None),
        P("sub", None, None),
        P("sub", None, None),
        P(),
        P(),
        P(),
    )
    return jax.shard_map(
        on_device,
        mesh=mesh,
        in_specs=placed,
        out_specs=(P("sub", None, None), P("sub", None, None)),
        check_vma=False,
    )
```

```python
import functools

import jax
import jax.numpy as jnp
from jax import lax
from jax.experimental import pallas as pl
from jax.experimental.pallas import tpu as pltpu
from jax.sharding import PartitionSpec as P

MESH = pl.DeviceIdType.MESH
PAD = 8
LANES = 128


def split(x):
    hi = x.astype(jnp.bfloat16)
    lo = (x - hi.astype(jnp.float32)).astype(jnp.bfloat16)
    return hi, lo


def mm(a, b):
    return jnp.dot(a, b, preferred_element_type=jnp.float32)


def mt(a, b):
    return lax.dot_general(
        a, b, (((1,), (1,)), ((), ())), preferred_element_type=jnp.float32
    )


def fold(x):
    out = None
    for y in range(0, x.shape[0], 8):
        for at in range(0, x.shape[1], LANES):
            piece = x[y : y + 8, at : at + LANES]
            out = piece if out is None else out + piece
    return out


def flip(i, mask):
    out, bit = i, 1
    while bit <= mask:
        if mask & bit:
            out = out + bit - 2 * bit * lax.rem(lax.div(i, bit), 2)
        bit *= 2
    return out


def drain(ref, sem):
    pltpu.make_async_copy(ref, ref, sem).wait()


def kernel(
    n, block,
    r_hbm, sg_hbm, wd_hbm, li_hbm, by_hbm, bz_hbm, gm_hbm,
    r, u1, u2, w1, w2, coef,
    sg, wd, wde, lf, by, bz, gm, lh, ll, by3, byt, bzp, bz6, fc,
    sp, sb, sa, ys, yh, yl, hs, hr,
    own, gat, tot, allb, low_s, low_r, nbr, gs, ggat,
    in_sem, as_, ar, bs, br, ls, lr, hss, hsr, gss, gsr, ready, go,
):
    layers, rows, depth = r.shape
    ky = by.shape[0]
    half = ky // 2
    kz = bz.shape[0]
    levels = gm.shape[0]
    blocks = n // block
    low_levels = block.bit_length() - 1
    quarter = rows // 4
    spans = (slice(0, quarter), slice(quarter, rows))
    me = lax.axis_index("sub")
    p = lax.rem(me, block)
    z = lax.div(me, block)
    us = (u1, u2)
    ws = (w1, w2)
    f32 = jnp.float32

    def load(i, src, dst):
        c = pltpu.make_async_copy(src, dst, in_sem.at[i])
        c.start()
        return c

    c_r = load(0, r_hbm, r)
    c_bz = load(1, bz_hbm, bz)
    c_by = load(2, by_hbm, by)
    c_l = load(3, li_hbm, lf)
    c_gm = load(4, gm_hbm, gm)

    barrier = pltpu.get_barrier_semaphore()
    in_block = [z * block + flip(p, d) for d in range(block - 1, 0, -1)]
    across = [lax.rem(z + d, blocks) * block + p for d in range(1, blocks)]
    first_cross = jnp.logical_and(p == 0, z > 0)
    last_cross = jnp.logical_and(p == block - 1, z < blocks - 1)

    late_down = jnp.logical_and(p == block - 2, z > 0)
    late_up = jnp.logical_and(p == 1, z < blocks - 1)

    def signal(target):
        pl.semaphore_signal(barrier, inc=1, device_id=(target,), device_id_type=MESH)

    for target in in_block + across:
        signal(target)

    @pl.when(first_cross)
    def _():
        signal(me - 1)

    @pl.when(last_cross)
    def _():
        signal(me + 1)

    zero_rows = jnp.zeros((PAD, depth), f32)
    for u in us:
        for l in range(layers):
            u[l, 0:PAD, :] = zero_rows
            u[l, PAD + rows : PAD + rows + PAD, :] = zero_rows
    sp[0:PAD, :] = zero_rows
    sp[PAD + rows : PAD + rows + PAD, :] = zero_rows

    @pl.when(me == 0)
    def _():
        hr[:, 0] = jnp.zeros((2, rows, depth), f32)

    @pl.when(me == n - 1)
    def _():
        hr[:, 1] = jnp.zeros((2, rows, depth), f32)

    def send(src, dst, s, q, target):
        return pltpu.make_async_remote_copy(
            src_ref=src, dst_ref=dst, send_sem=s, recv_sem=q,
            device_id=(target,), device_id_type=MESH,
        )

    def project(k):
        hi, lo = yh[...], yl[...]
        bh, bl = bzp[0 : 2 * kz], bzp[2 * kz : 4 * kz]
        part = mt(hi, bh) + mt(lo, bh) + mt(hi, bl)
        ph, pl_ = split(part)
        bh, bl = by3[0:ky], by3[ky : 2 * ky]
        full = mm(bh, ph) + mm(bh, pl_) + mm(bl, ph)
        lane = lax.broadcasted_iota(jnp.int32, (half, 2 * kz), 1)
        packed = jnp.where(lane < kz, full[0:half], full[half:ky])
        own[k] = packed
        gat[k, p] = packed

    def a_send(k):
        for target in in_block:
            send(own.at[k], gat.at[k, p], as_.at[k], ar.at[k], target).start()
        pl.semaphore_signal(
            ready.at[k], inc=1, device_id=(in_block[-1],), device_id_type=MESH
        )

    def a_wait(k, sem):
        drain(gat.at[k, pl.ds(0, block - 1)], sem.at[k])

    def b_send(k):
        for target in across:
            send(tot.at[k], allb.at[k, z], bs.at[k], br.at[k], target).start()

    def b_wait(k, sem):
        if blocks > 1:
            drain(allb.at[k, pl.ds(0, blocks - 1)], sem.at[k])

    def piece(ref, k, way, c):
        at = spans[c]
        return ref.at[k, way, pl.ds(at.start, at.stop - at.start)]

    def down(k, c):
        return send(
            piece(hs, k, 0, c), piece(hr, k, 1, c), hss.at[k, 0], hsr.at[k, 1, c], me - 1
        )

    def up(k, c):
        return send(
            piece(hs, k, 1, c), piece(hr, k, 0, c), hss.at[k, 1], hsr.at[k, 0, c], me + 1
        )

    def low_down(k):
        return send(low_s.at[k, 0], low_r.at[k, 1], ls.at[k, 0], lr.at[k, 1], me - block)

    def low_up(k):
        return send(low_s.at[k, 1], low_r.at[k, 0], ls.at[k, 1], lr.at[k, 0], me + block)

    def allow(k, way, target):
        pl.semaphore_signal(
            go.at[k, way], inc=1, device_id=(target,), device_id_type=MESH
        )

    def cross(k):
        @pl.when(first_cross)
        def _():
            pl.semaphore_wait(go.at[k, 0], 1)
            for c in range(2):
                down(k, c).start()

        @pl.when(last_cross)
        def _():
            pl.semaphore_wait(go.at[k, 1], 1)
            for c in range(2):
                up(k, c).start()

    def later(k):
        @pl.when(late_down)
        def _():
            down(k, 1).start()

        @pl.when(late_up)
        def _():
            up(k, 1).start()

    def edges(k, field):
        u = us[k]
        xh, xl = split(jnp.concatenate([field[0], field[layers - 1]], axis=0))
        out = mm(xh, lh[...]) + mm(xl, lh[...]) + mm(xh, ll[...])
        first, last = out[0:rows], out[rows : 2 * rows]
        hs[k, 0] = first
        hs[k, 1] = last
        u[0, PAD : PAD + rows] = first
        u[layers - 1, PAD : PAD + rows] = last

    def greet(k):
        pl.semaphore_wait(ready.at[k], 1)

        @pl.when(jnp.logical_and(p == block - 1, z > 0))
        def _():
            allow(k, 1, me - block)

        @pl.when(jnp.logical_and(p == 0, z < blocks - 1))
        def _():
            allow(k, 0, me + block)

    def issue(k, c):
        downs, ups = p > 0, p < block - 1
        if c == 1:
            downs = jnp.logical_and(downs, jnp.logical_not(late_down))
            ups = jnp.logical_and(ups, jnp.logical_not(late_up))

        @pl.when(downs)
        def _():
            down(k, c).start()

        @pl.when(ups)
        def _():
            up(k, c).start()

    def middle(k, field):
        u = us[k]
        inner = range(1, layers - 1)
        xh, xl = split(jnp.concatenate([field[l] for l in inner], axis=0))
        out = mm(xh, lh[...]) + mm(xl, lh[...]) + mm(xh, ll[...])
        for i, l in enumerate(inner):
            u[l, PAD : PAD + rows, :] = out[i * rows : (i + 1) * rows]

    def low_part(k, q):
        out = None
        for level in range(low_levels):
            width = 2 ** (level + 1)
            start = lax.div(q, width) * width
            if width == block:
                acc = tot[k]
            else:
                acc = gat[k, start]
                for j in range(1, width):
                    acc = acc + gat[k, start + j]
            term = fc[level] * acc
            out = term if out is None else out + term
        return out

    def high_part(k, zz):
        out = None
        for level in range(low_levels, levels):
            width = 2 ** (level + 1) // block
            start = lax.div(zz, width) * width
            acc = allb[k, start]
            for j in range(1, width):
                acc = acc + allb[k, start + j]
            term = fc[level] * acc
            out = term if out is None else out + term
        return jnp.zeros(tot.shape[1:], f32) if out is None else out

    def exchange(k):
        a_wait(k, ar)
        acc = gat[k, 0]
        for j in range(1, block):
            acc = acc + gat[k, j]
        tot[k] = acc
        allb[k, z] = acc
        b_send(k)

        @pl.when(jnp.logical_and(p == block - 1, z > 0))
        def _():
            low_s[k, 0] = low_part(k, 0)
            low_down(k).start()

        @pl.when(jnp.logical_and(p == 0, z < blocks - 1))
        def _():
            low_s[k, 1] = low_part(k, block - 1)
            low_up(k).start()

        nbr[0] = low_part(k, jnp.maximum(p - 1, 0))
        nbr[1] = low_part(k, p)
        nbr[2] = low_part(k, jnp.minimum(p + 1, block - 1))

        @pl.when(first_cross)
        def _():
            low_up(k).wait_recv()
            nbr[0] = low_r[k, 0]

        @pl.when(last_cross)
        def _():
            low_down(k).wait_recv()
            nbr[2] = low_r[k, 1]

    def back(k):
        b_wait(k, br)
        here = nbr[1] + high_part(k, z)
        before = nbr[0] + high_part(k, lax.div(jnp.maximum(me - 1, 0), block))
        after = nbr[2] + high_part(k, lax.div(jnp.minimum(me + 1, n - 1), block))
        before = jnp.where(me > 0, before, 0.0)
        after = jnp.where(me < n - 1, after, 0.0)
        lane = lax.broadcasted_iota(jnp.int32, (half, 2 * kz), 1)
        three = []
        for c in (here, before, after):
            three += [jnp.where(lane < kz, c, 0.0), jnp.where(lane < kz, 0.0, c)]
        th, tl = split(jnp.concatenate(three, axis=0))
        out = mm(jnp.concatenate([th, tl, th], axis=1), bz6[...])
        th, tl = split(out)
        spreads = []
        for j in range(3):
            piece = slice(j * ky, (j + 1) * ky)
            spreads.append(
                mm(byt[...], jnp.concatenate([th[piece], tl[piece], th[piece]], axis=0))
            )
        sp[PAD : PAD + rows, :] = spreads[0]
        sb[...] = spreads[1]
        sa[...] = spreads[2]

    step = 32

    def beside(ref, l, y):
        a = PAD + y
        here = (lambda s: ref[s, :]) if l is None else (lambda s: ref[l, s, :])
        c = here(slice(a, a + step))
        col = lax.broadcasted_iota(jnp.int32, (step, depth), 1)
        fwd = jnp.where(col == depth - 1, 0.0, pltpu.roll(c, depth - 1, 1))
        bwd = jnp.where(col == 0, 0.0, pltpu.roll(c, 1, 1))
        ups = here(slice(a + 1, a + step + 1))
        downs = here(slice(a - 1, a + step - 1))
        return c, ups + downs + fwd + bwd

    def inner_image(k, which):
        u = us[k]
        for l in which:
            for y in range(0, rows, step):
                a = PAD + y
                at = slice(y, y + step)
                c, around = beside(u, l, y)
                diag = sg[l, at, :] + (4.0 if k == 0 else 0.0)
                out = (2.0 + diag) * c - around
                if k == 0:
                    sg[l, at, :] = diag
                wind = wd[l, at, :]
                if l < layers - 1:
                    out = out + (wind - 1.0) * u[l + 1, a : a + step, :]
                if l > 0:
                    out = out - (wind + 1.0) * u[l - 1, a : a + step, :]
                if k == 0 and l == 0:
                    wde[0, at, :] = wind + 1.0
                if k == 0 and l == layers - 1:
                    wde[1, at, :] = wind - 1.0
                ws[k][l, at, :] = out

    def tally(totals, l, at, out):
        for i, other in enumerate((r, w1, None)):
            other = out if other is None else other[l, at, :]
            term = fold(other * out)
            totals[i] = term if totals[i] is None else totals[i] + term

    outer = (0,) if layers == 1 else (0, layers - 1)

    def image(k, totals):
        w = ws[k]
        for y in range(0, rows, step):
            at = slice(y, y + step)
            s, around = beside(sp, None, y)
            total = None
            for l in range(layers):
                out = w[l, at, :] + (sg[l, at, :] * s - around)
                if l == 0:
                    out = out + wde[0, at, :] * (s - sb[at, :])
                if l == layers - 1:
                    out = out + wde[1, at, :] * (sa[at, :] - s)
                w[l, at, :] = out
                total = out if total is None else total + out
                if k == 1 and l not in outer:
                    tally(totals, l, at, out)
            if k == 0:
                ys[at, :] = total

    def meet(k, c, totals):
        w = ws[k]

        @pl.when(me > 0)
        def _():
            up(k, c).wait_recv()

        @pl.when(me < n - 1)
        def _():
            down(k, c).wait_recv()

        for y in range(spans[c].start, spans[c].stop, quarter):
            at = slice(y, y + quarter)
            change = (-(wde[0, at, :] * hr[k, 0, at, :]), wde[1, at, :] * hr[k, 1, at, :])
            if layers == 1:
                change = (change[0] + change[1],)
            for l, more in zip(outer, change):
                out = w[l, at, :] + more
                w[l, at, :] = out
                if k == 1:
                    tally(totals, l, at, out)
            if k == 0:
                total = ys[at, :]
                for more in change:
                    total = total + more
                yh[at, :], yl[at, :] = split(total)

    def place(totals, first):
        lane = lax.broadcasted_iota(jnp.int32, (8, LANES), 1)
        out = jnp.zeros((8, LANES), f32)
        for i, t in enumerate(totals):
            out = jnp.where(lane == first + i, jnp.sum(t, axis=1, keepdims=True), out)
        return out

    def dots(pairs):
        out = []
        for a, b in pairs:
            acc = None
            for l in range(layers):
                term = fold(a[l] * b[l])
                acc = term if acc is None else acc + term
            out.append(acc)
        return out

    def add_spread(k):
        u = us[k]
        for y in range(0, rows, step):
            s = sp[PAD + y : PAD + y + step, :]
            for l in range(layers):
                u[l, PAD + y : PAD + y + step, :] = u[l, PAD + y : PAD + y + step, :] + s

    c_bz.wait()
    hi, lo = split(bz[...])
    for j in range(2):
        bzp[j * kz : (j + 1) * kz] = hi
        bzp[(2 + j) * kz : (3 + j) * kz] = lo
    for j in range(4):
        bz6[j * kz : (j + 1) * kz] = hi
    for j in range(4, 6):
        bz6[j * kz : (j + 1) * kz] = lo
    c_by.wait()
    hi, lo = split(by[...])
    by3[0:ky] = hi
    by3[ky : 2 * ky] = lo
    c_r.wait()
    for y in range(0, rows, step):
        at = slice(y, y + step)
        total = r[0, at, :]
        for l in range(1, layers):
            total = total + r[l, at, :]
        yh[at, :], yl[at, :] = split(total)
    project(0)
    extra = jnp.where(first_cross, 1, 0) + jnp.where(last_cross, 1, 0)
    pl.semaphore_wait(barrier, block - 1 + blocks - 1 + extra)
    a_send(0)
    c_l.wait()
    c_sg = load(5, sg_hbm, sg)
    c_wd = load(6, wd_hbm, wd)
    big, small = split(lf[0])
    lh[...] = big
    ll[...] = small
    edges(0, r)
    greet(0)
    issue(0, 0)
    issue(0, 1)
    cross(0)
    middle(0, r)
    c_gm.wait()
    for level in range(levels):
        g = gm[level]
        fc[level] = jnp.concatenate([g[0:half], g[half:ky]], axis=1) * (
            (layers * 2 ** (level + 1)) ** -0.5
        )
    hi, lo = split(by[...].T)
    byt[...] = jnp.concatenate([hi, hi, lo], axis=1)
    c_sg.wait()
    c_wd.wait()
    inner_image(0, range(1))
    later(0)
    inner_image(0, range(1, layers))
    exchange(0)
    back(0)
    image(0, None)
    meet(0, 0, None)
    meet(0, 1, None)
    project(1)
    a_send(1)
    edges(1, w1)
    greet(1)
    issue(1, 0)
    issue(1, 1)
    cross(1)
    middle(1, w1)
    add_spread(0)
    inner_image(1, range(1))
    later(1)
    inner_image(1, range(1, layers))
    early = place(dots([(r, r), (r, w1), (w1, w1)]), 0)
    exchange(1)
    back(1)
    totals = [None] * 3
    image(1, totals)
    meet(1, 0, totals)
    meet(1, 1, totals)
    late = place(totals, 3)
    flat = jnp.sum(early + late, axis=0, keepdims=True)
    gs[...] = flat
    ggat[me] = flat
    for d in range(n - 1, 0, -1):
        send(gs, ggat.at[me], gss, gsr, flip(me, d)).start()

    add_spread(1)
    for k in range(2):
        a_wait(k, as_)
        b_wait(k, bs)

        @pl.when(jnp.logical_and(p == block - 1, z > 0))
        def _():
            low_down(k).wait_send()

        @pl.when(jnp.logical_and(p == 0, z < blocks - 1))
        def _():
            low_up(k).wait_send()

        @pl.when(me > 0)
        def _():
            drain(hs.at[k, 0], hss.at[k, 0])

        @pl.when(me < n - 1)
        def _():
            drain(hs.at[k, 1], hss.at[k, 1])

    drain(ggat.at[pl.ds(0, n - 1)], gss)
    drain(ggat.at[pl.ds(0, n - 1)], gsr)
    total = jnp.sum(ggat[...], axis=0)
    g01, g11, g02, g12, g22 = (
        jnp.broadcast_to(total[:, j : j + 1], (1, LANES)) for j in range(1, 6)
    )
    ratio = g12 / g11
    c2 = (g02 - ratio * g01) / (g22 - ratio * g12)
    c1 = g01 / g11 - ratio * c2
    coef[0] = jnp.broadcast_to(c1, (8, LANES))
    coef[1] = jnp.broadcast_to(c2, (8, LANES))


def finish(r, u1, u2, w1, w2, coef, x_hbm, res_hbm, xo, ro, x_sem, res_sem):
    layers, rows, depth = r.shape
    step = 8
    c1 = jnp.concatenate([coef[0]] * (depth // LANES), axis=1)
    c2 = jnp.concatenate([coef[1]] * (depth // LANES), axis=1)
    for l in range(layers):
        for y in range(0, rows, step):
            a = PAD + y
            xo[l, y : y + step, :] = (
                c1 * u1[l, a : a + step, :] + c2 * u2[l, a : a + step, :]
            )
        pltpu.make_async_copy(xo.at[l], x_hbm.at[l], x_sem).start()
    for l in range(layers):
        for y in range(0, rows, step):
            ro[l, y : y + step, :] = (
                r[l, y : y + step, :]
                - c1 * w1[l, y : y + step, :] - c2 * w2[l, y : y + step, :]
            )
        pltpu.make_async_copy(ro.at[l], res_hbm.at[l], res_sem).start()
    drain(xo, x_sem)
    drain(ro, res_sem)


def on_device(right_side, sigma, wind, local_inverse, basis_y, basis_z, gamma):
    n = lax.axis_size("sub")
    block = min(8, n)
    blocks = n // block
    layers, rows, depth = right_side.shape
    ky = basis_y.shape[1]
    kz = basis_z.shape[1]
    f32, bf16 = jnp.float32, jnp.bfloat16
    packed = (ky // 2, 2 * kz)
    cube = pltpu.VMEM((layers, rows, depth), f32)
    padded = pltpu.VMEM((layers, rows + 2 * PAD, depth), f32)
    plane = pltpu.VMEM((rows, depth), f32)
    halo = pltpu.VMEM((2, 2, rows, depth), f32)
    dma = pltpu.SemaphoreType.DMA
    scratch = [
        cube, cube,
        pltpu.VMEM((2, rows, depth), f32),
        pltpu.VMEM((1, depth, depth), f32),
        pltpu.VMEM((ky, rows), f32),
        pltpu.VMEM((kz, depth), f32),
        pltpu.VMEM(gamma.shape, f32),
        pltpu.VMEM((depth, depth), bf16),
        pltpu.VMEM((depth, depth), bf16),
        pltpu.VMEM((2 * ky, rows), bf16),
        pltpu.VMEM((rows, 3 * ky), bf16),
        pltpu.VMEM((4 * kz, depth), bf16),
        pltpu.VMEM((6 * kz, depth), bf16),
        pltpu.VMEM((gamma.shape[0],) + packed, f32),
        pltpu.VMEM((rows + 2 * PAD, depth), f32),
        plane, plane, plane,
        pltpu.VMEM((rows, depth), bf16),
        pltpu.VMEM((rows, depth), bf16),
        halo, halo,
        pltpu.VMEM((2,) + packed, f32),
        pltpu.VMEM((2, block) + packed, f32),
        pltpu.VMEM((2,) + packed, f32),
        pltpu.VMEM((2, blocks) + packed, f32),
        pltpu.VMEM((2, 2) + packed, f32),
        pltpu.VMEM((2, 2) + packed, f32),
        pltpu.VMEM((3,) + packed, f32),
        pltpu.VMEM((1, LANES), f32),
        pltpu.VMEM((n, 1, LANES), f32),
        dma((7,)),
        dma((2,)), dma((2,)),
        dma((2,)), dma((2,)),
        dma((2, 2)), dma((2, 2)),
        dma((2, 2)), dma((2, 2, 2)),
        dma, dma,
        pltpu.SemaphoreType.REGULAR((2,)),
        pltpu.SemaphoreType.REGULAR((2, 2)),
    ]
    hbm = pl.BlockSpec(memory_space=pltpu.HBM)
    vmem = pl.BlockSpec(memory_space=pltpu.VMEM)
    out = jax.ShapeDtypeStruct(right_side.shape, f32)
    pieces = pl.pallas_call(
        functools.partial(kernel, n, block),
        out_shape=(cube, padded, padded, cube, cube, pltpu.VMEM((2, 8, LANES), f32)),
        in_specs=[hbm] * 7,
        out_specs=(vmem,) * 6,
        scratch_shapes=scratch,
        compiler_params=pltpu.CompilerParams(
            collective_id=0, has_side_effects=True, vmem_limit_bytes=50 * 2**20,
        ),
        name="gmres",
    )(right_side, sigma, wind, local_inverse, basis_y.T, basis_z.T, gamma)
    return pl.pallas_call(
        finish,
        out_shape=(out, out),
        in_specs=[vmem] * 6,
        out_specs=(hbm, hbm),
        scratch_shapes=[cube, cube, dma, dma],
        compiler_params=pltpu.CompilerParams(vmem_limit_bytes=24 * 2**20),
        name="finish",
    )(*pieces)


def solution(mesh):
    placed = (
        P("sub", None, None),
        P("sub", None, None),
        P("sub", None, None),
        P("sub", None, None),
        P(),
        P(),
        P(),
    )
    return jax.shard_map(
        on_device,
        mesh=mesh,
        in_specs=placed,
        out_specs=(P("sub", None, None), P("sub", None, None)),
        check_vma=False,
    )
```

```python
import functools

import jax
import jax.numpy as jnp
from jax import lax
from jax.experimental import pallas as pl
from jax.experimental.pallas import tpu as pltpu
from jax.sharding import PartitionSpec as P

MESH = pl.DeviceIdType.MESH
PAD = 8
LANES = 128


def split(x):
    hi = x.astype(jnp.bfloat16)
    lo = (x - hi.astype(jnp.float32)).astype(jnp.bfloat16)
    return hi, lo


def mm(a, b):
    return jnp.dot(a, b, preferred_element_type=jnp.float32)


def mt(a, b):
    return lax.dot_general(
        a, b, (((1,), (1,)), ((), ())), preferred_element_type=jnp.float32
    )


def fold(x):
    out = None
    for y in range(0, x.shape[0], 8):
        for at in range(0, x.shape[1], LANES):
            piece = x[y : y + 8, at : at + LANES]
            out = piece if out is None else out + piece
    return out


def flip(i, mask):
    out, bit = i, 1
    while bit <= mask:
        if mask & bit:
            out = out + bit - 2 * bit * lax.rem(lax.div(i, bit), 2)
        bit *= 2
    return out


def drain(ref, sem):
    pltpu.make_async_copy(ref, ref, sem).wait()


def kernel(
    n, block,
    r_hbm, sg_hbm, wd_hbm, li_hbm, by_hbm, bz_hbm, gm_hbm,
    r, u1, u2, w1, w2, coef,
    sg, wd, wde, lf, by, bz, gm, lh, ll, by3, byt, bzp, bz6, fc,
    sp, sb, sa, ys, yh, yl, hs, hr,
    own, gat, tot, allb, low_s, low_r, nbr, gs, ggat,
    in_sem, as_, ar, bs, br, ls, lr, hss, hsr, gss, gsr, ready, go,
):
    layers, rows, depth = r.shape
    ky = by.shape[0]
    half = ky // 2
    kz = bz.shape[0]
    levels = gm.shape[0]
    blocks = n // block
    low_levels = block.bit_length() - 1
    quarter = rows // 8
    spans = (slice(0, quarter), slice(quarter, rows))
    me = lax.axis_index("sub")
    p = lax.rem(me, block)
    z = lax.div(me, block)
    us = (u1, u2)
    ws = (w1, w2)
    f32 = jnp.float32

    def load(i, src, dst):
        c = pltpu.make_async_copy(src, dst, in_sem.at[i])
        c.start()
        return c

    c_r = load(0, r_hbm, r)
    c_bz = load(1, bz_hbm, bz)
    c_by = load(2, by_hbm, by)
    c_l = load(3, li_hbm, lf)
    c_gm = load(4, gm_hbm, gm)

    barrier = pltpu.get_barrier_semaphore()
    in_block = [z * block + flip(p, d) for d in range(block - 1, 0, -1)]
    across = [lax.rem(z + d, blocks) * block + p for d in range(1, blocks)]
    beyond = [lax.rem(z + d, blocks) * block + flip(p, 1) for d in range(1, blocks)]
    odd = lax.rem(p, 2) == 1
    even = jnp.logical_not(odd)
    way = lax.rem(p, 2)
    far, near = way * (layers - 1), (1 - way) * (layers - 1)
    speaks = jnp.logical_or(jnp.logical_and(odd, p < block - 1), p == block - 2)
    first_cross = jnp.logical_and(p == 0, z > 0)
    last_cross = jnp.logical_and(p == block - 1, z < blocks - 1)

    late_down = jnp.logical_and(p == block - 2, z > 0)
    late_up = jnp.logical_and(p == 1, z < blocks - 1)

    def signal(target):
        pl.semaphore_signal(barrier, inc=1, device_id=(target,), device_id_type=MESH)

    for target in in_block + across + beyond:
        signal(target)

    @pl.when(first_cross)
    def _():
        signal(me - 1)

    @pl.when(last_cross)
    def _():
        signal(me + 1)

    zero_rows = jnp.zeros((PAD, depth), f32)
    for u in us:
        for l in range(layers):
            u[l, 0:PAD, :] = zero_rows
            u[l, PAD + rows : PAD + rows + PAD, :] = zero_rows
    sp[0:PAD, :] = zero_rows
    sp[PAD + rows : PAD + rows + PAD, :] = zero_rows

    @pl.when(me == 0)
    def _():
        hr[:, 0] = jnp.zeros((2, rows, depth), f32)

    @pl.when(me == n - 1)
    def _():
        hr[:, 1] = jnp.zeros((2, rows, depth), f32)

    def send(src, dst, s, q, target):
        return pltpu.make_async_remote_copy(
            src_ref=src, dst_ref=dst, send_sem=s, recv_sem=q,
            device_id=(target,), device_id_type=MESH,
        )

    def project(k):
        hi, lo = yh[...], yl[...]
        top = mm(by3[...], hi)
        part = top[0:ky] + top[ky : 2 * ky] + mm(by3[0:ky], lo)
        ph, pl_ = split(part)
        bh, bl = bzp[0 : 2 * kz], bzp[2 * kz : 4 * kz]
        top = mt(jnp.concatenate([ph, pl_], axis=0), bh)
        full = top[0:ky] + top[ky : 2 * ky] + mt(ph, bl)
        lane = lax.broadcasted_iota(jnp.int32, (half, 2 * kz), 1)
        packed = jnp.where(lane < kz, full[0:half], full[half:ky])
        own[k] = packed
        gat[k, p] = packed

    def a_send(k):
        for target in in_block:
            send(own.at[k], gat.at[k, p], as_.at[k], ar.at[k], target).start()
        pl.semaphore_signal(
            ready.at[k], inc=1, device_id=(in_block[-1],), device_id_type=MESH
        )

    def a_wait(k, sem):
        drain(gat.at[k, pl.ds(0, block - 1)], sem.at[k])

    def b_send(k):
        @pl.when(speaks)
        def _():
            for target in across + beyond:
                send(tot.at[k], allb.at[k, z], bs.at[k], br.at[k], target).start()

    def b_wait(k, sem):
        if blocks > 1:
            drain(allb.at[k, pl.ds(0, blocks - 1)], sem.at[k])

    def piece(ref, k, way, c):
        at = spans[c]
        return ref.at[k, way, pl.ds(at.start, at.stop - at.start)]

    def down(k, c):
        return send(
            piece(hs, k, 0, c), piece(hr, k, 1, c), hss.at[k, 0], hsr.at[k, 1, c], me - 1
        )

    def up(k, c):
        return send(
            piece(hs, k, 1, c), piece(hr, k, 0, c), hss.at[k, 1], hsr.at[k, 0, c], me + 1
        )

    def low_down(k):
        return send(low_s.at[k, 0], low_r.at[k, 1], ls.at[k, 0], lr.at[k, 1], me - block)

    def low_up(k):
        return send(low_s.at[k, 1], low_r.at[k, 0], ls.at[k, 1], lr.at[k, 0], me + block)

    def allow(k, way, target):
        pl.semaphore_signal(
            go.at[k, way], inc=1, device_id=(target,), device_id_type=MESH
        )

    def cross(k):
        @pl.when(first_cross)
        def _():
            pl.semaphore_wait(go.at[k, 0], 1)
            for c in range(2):
                down(k, c).start()

        @pl.when(last_cross)
        def _():
            pl.semaphore_wait(go.at[k, 1], 1)
            for c in range(2):
                up(k, c).start()

    def later(k):
        @pl.when(late_down)
        def _():
            down(k, 1).start()

        @pl.when(late_up)
        def _():
            up(k, 1).start()

    def times(x):
        xh, xl = split(x)
        m = x.shape[0]
        both = mm(jnp.concatenate([xh, xl], axis=0), lh[...])
        return both[0:m] + both[m : 2 * m] + mm(xh, ll[...])

    def far_edge(k, field, at):
        out = times(field[far, at])
        hs[k, way, at] = out
        us[k][far, PAD + at.start : PAD + at.stop] = out

    def others(k, field):
        inner = range(1, layers - 1)
        out = times(jnp.concatenate([field[near]] + [field[l] for l in inner], axis=0))
        hs[k, 1 - way] = out[0:rows]
        us[k][near, PAD : PAD + rows] = out[0:rows]
        for i, l in enumerate(inner):
            us[k][l, PAD : PAD + rows, :] = out[(i + 1) * rows : (i + 2) * rows]

    def greet(k):
        pl.semaphore_wait(ready.at[k], 1)

        @pl.when(jnp.logical_and(p == block - 1, z > 0))
        def _():
            allow(k, 1, me - block)

        @pl.when(jnp.logical_and(p == 0, z < blocks - 1))
        def _():
            allow(k, 0, me + block)

    def issue(k, c):
        downs, ups = jnp.logical_and(even, p > 0), jnp.logical_and(odd, p < block - 1)
        if c == 1:
            downs = jnp.logical_and(downs, jnp.logical_not(late_down))
            ups = jnp.logical_and(ups, jnp.logical_not(late_up))

        @pl.when(downs)
        def _():
            down(k, c).start()

        @pl.when(ups)
        def _():
            up(k, c).start()

    def issue_near(k):
        @pl.when(even)
        def _():
            for c in range(2):
                up(k, c).start()

        @pl.when(odd)
        def _():
            for c in range(2):
                down(k, c).start()

    def low_part(k, q):
        out = None
        for level in range(low_levels):
            width = 2 ** (level + 1)
            start = lax.div(q, width) * width
            if width == block:
                acc = tot[k]
            else:
                acc = gat[k, start]
                for j in range(1, width):
                    acc = acc + gat[k, start + j]
            term = fc[level] * acc
            out = term if out is None else out + term
        return out

    def high_part(k, zz):
        out = None
        for level in range(low_levels, levels):
            width = 2 ** (level + 1) // block
            start = lax.div(zz, width) * width
            acc = allb[k, start]
            for j in range(1, width):
                acc = acc + allb[k, start + j]
            term = fc[level] * acc
            out = term if out is None else out + term
        return jnp.zeros(tot.shape[1:], f32) if out is None else out

    def exchange(k):
        a_wait(k, ar)
        acc = gat[k, 0]
        for j in range(1, block):
            acc = acc + gat[k, j]
        tot[k] = acc
        allb[k, z] = acc
        b_send(k)

        @pl.when(jnp.logical_and(p == block - 1, z > 0))
        def _():
            low_s[k, 0] = low_part(k, 0)
            low_down(k).start()

        @pl.when(jnp.logical_and(p == 0, z < blocks - 1))
        def _():
            low_s[k, 1] = low_part(k, block - 1)
            low_up(k).start()

        nbr[0] = low_part(k, jnp.maximum(p - 1, 0))
        nbr[1] = low_part(k, p)
        nbr[2] = low_part(k, jnp.minimum(p + 1, block - 1))

        @pl.when(first_cross)
        def _():
            low_up(k).wait_recv()
            nbr[0] = low_r[k, 0]

        @pl.when(last_cross)
        def _():
            low_down(k).wait_recv()
            nbr[2] = low_r[k, 1]

    def back(k):
        b_wait(k, br)
        here = nbr[1] + high_part(k, z)
        before = nbr[0] + high_part(k, lax.div(jnp.maximum(me - 1, 0), block))
        after = nbr[2] + high_part(k, lax.div(jnp.minimum(me + 1, n - 1), block))
        before = jnp.where(me > 0, before, 0.0)
        after = jnp.where(me < n - 1, after, 0.0)
        lane = lax.broadcasted_iota(jnp.int32, (half, 2 * kz), 1)
        three = []
        for c in (here, before, after):
            three += [jnp.where(lane < kz, c, 0.0), jnp.where(lane < kz, 0.0, c)]
        th, tl = split(jnp.concatenate(three, axis=0))
        out = mm(jnp.concatenate([th, tl, th], axis=1), bz6[...])
        th, tl = split(out)
        spreads = []
        for j in range(3):
            piece = slice(j * ky, (j + 1) * ky)
            spreads.append(
                mm(byt[...], jnp.concatenate([th[piece], tl[piece], th[piece]], axis=0))
            )
        sp[PAD : PAD + rows, :] = spreads[0]
        sb[...] = spreads[1]
        sa[...] = spreads[2]

    step = 32

    def beside(ref, l, y):
        a = PAD + y
        here = (lambda s: ref[s, :]) if l is None else (lambda s: ref[l, s, :])
        c = here(slice(a, a + step))
        col = lax.broadcasted_iota(jnp.int32, (step, depth), 1)
        fwd = jnp.where(col == depth - 1, 0.0, pltpu.roll(c, depth - 1, 1))
        bwd = jnp.where(col == 0, 0.0, pltpu.roll(c, 1, 1))
        ups = here(slice(a + 1, a + step + 1))
        downs = here(slice(a - 1, a + step - 1))
        return c, ups + downs + fwd + bwd

    def inner_image(k, which):
        u = us[k]
        for l in which:
            for y in range(0, rows, step):
                a = PAD + y
                at = slice(y, y + step)
                c, around = beside(u, l, y)
                diag = sg[l, at, :] + (4.0 if k == 0 else 0.0)
                out = (2.0 + diag) * c - around
                if k == 0:
                    sg[l, at, :] = diag
                wind = wd[l, at, :]
                if l < layers - 1:
                    out = out + (wind - 1.0) * u[l + 1, a : a + step, :]
                if l > 0:
                    out = out - (wind + 1.0) * u[l - 1, a : a + step, :]
                if k == 0 and l == 0:
                    wde[0, at, :] = wind + 1.0
                if k == 0 and l == layers - 1:
                    wde[1, at, :] = wind - 1.0
                ws[k][l, at, :] = out

    def tally(totals, l, at, out):
        for i, other in enumerate((r, w1, None)):
            other = out if other is None else other[l, at, :]
            term = fold(other * out)
            totals[i] = term if totals[i] is None else totals[i] + term

    outer = (0,) if layers == 1 else (0, layers - 1)

    def image(k, totals):
        w = ws[k]
        for y in range(0, rows, step):
            at = slice(y, y + step)
            s, around = beside(sp, None, y)
            total = None
            for l in range(layers):
                out = w[l, at, :] + (sg[l, at, :] * s - around)
                if l == 0:
                    out = out + wde[0, at, :] * (s - sb[at, :])
                if l == layers - 1:
                    out = out + wde[1, at, :] * (sa[at, :] - s)
                w[l, at, :] = out
                total = out if total is None else total + out
                if k == 1 and l not in outer:
                    tally(totals, l, at, out)
            if k == 0:
                ys[at, :] = total

    def meet(k, c, totals):
        w = ws[k]

        @pl.when(me > 0)
        def _():
            up(k, c).wait_recv()

        @pl.when(me < n - 1)
        def _():
            down(k, c).wait_recv()

        for y in range(spans[c].start, spans[c].stop, quarter):
            at = slice(y, y + quarter)
            change = (-(wde[0, at, :] * hr[k, 0, at, :]), wde[1, at, :] * hr[k, 1, at, :])
            if layers == 1:
                change = (change[0] + change[1],)
            for l, more in zip(outer, change):
                out = w[l, at, :] + more
                w[l, at, :] = out
                if k == 1:
                    tally(totals, l, at, out)
            if k == 0:
                total = ys[at, :]
                for more in change:
                    total = total + more
                yh[at, :], yl[at, :] = split(total)

    def place(totals, first):
        lane = lax.broadcasted_iota(jnp.int32, (8, LANES), 1)
        out = jnp.zeros((8, LANES), f32)
        for i, t in enumerate(totals):
            out = jnp.where(lane == first + i, jnp.sum(t, axis=1, keepdims=True), out)
        return out

    def dots(pairs):
        out = []
        for a, b in pairs:
            acc = None
            for l in range(layers):
                term = fold(a[l] * b[l])
                acc = term if acc is None else acc + term
            out.append(acc)
        return out

    def add_spread(k):
        u = us[k]
        for y in range(0, rows, step):
            s = sp[PAD + y : PAD + y + step, :]
            for l in range(layers):
                u[l, PAD + y : PAD + y + step, :] = u[l, PAD + y : PAD + y + step, :] + s

    c_bz.wait()
    hi, lo = split(bz[...])
    for j in range(2):
        bzp[j * kz : (j + 1) * kz] = hi
        bzp[(2 + j) * kz : (3 + j) * kz] = lo
    for j in range(4):
        bz6[j * kz : (j + 1) * kz] = hi
    for j in range(4, 6):
        bz6[j * kz : (j + 1) * kz] = lo
    c_by.wait()
    hi, lo = split(by[...])
    by3[0:ky] = hi
    by3[ky : 2 * ky] = lo
    c_r.wait()
    for y in range(0, rows, step):
        at = slice(y, y + step)
        total = r[0, at, :]
        for l in range(1, layers):
            total = total + r[l, at, :]
        yh[at, :], yl[at, :] = split(total)
    project(0)
    extra = jnp.where(first_cross, 1, 0) + jnp.where(last_cross, 1, 0)
    pl.semaphore_wait(barrier, block - 1 + 2 * (blocks - 1) + extra)
    a_send(0)
    c_l.wait()
    c_sg = load(5, sg_hbm, sg)
    c_wd = load(6, wd_hbm, wd)
    big, small = split(lf[0])
    lh[...] = big
    ll[...] = small
    far_edge(0, r, slice(0, rows))
    greet(0)
    issue(0, 0)
    issue(0, 1)
    cross(0)
    others(0, r)
    issue_near(0)
    c_gm.wait()
    for level in range(levels):
        g = gm[level]
        fc[level] = jnp.concatenate([g[0:half], g[half:ky]], axis=1) * (
            (layers * 2 ** (level + 1)) ** -0.5
        )
    hi, lo = split(by[...].T)
    byt[...] = jnp.concatenate([hi, hi, lo], axis=1)
    c_sg.wait()
    c_wd.wait()
    inner_image(0, range(1))
    later(0)
    inner_image(0, range(1, layers))
    exchange(0)
    back(0)
    image(0, None)
    meet(0, 0, None)
    far_edge(1, w1, spans[0])
    issue(1, 0)
    meet(0, 1, None)
    project(1)
    a_send(1)
    far_edge(1, w1, spans[1])
    greet(1)
    issue(1, 1)
    cross(1)
    others(1, w1)
    issue_near(1)
    add_spread(0)
    inner_image(1, range(1))
    later(1)
    inner_image(1, range(1, layers))
    early = place(dots([(r, r), (r, w1), (w1, w1)]), 0)
    exchange(1)
    back(1)
    totals = [None] * 3
    image(1, totals)
    meet(1, 0, totals)
    meet(1, 1, totals)
    late = place(totals, 3)
    flat = jnp.sum(early + late, axis=0, keepdims=True)
    gs[...] = flat
    ggat[me] = flat
    for d in range(n - 1, 0, -1):
        send(gs, ggat.at[me], gss, gsr, flip(me, d)).start()

    add_spread(1)
    for k in range(2):
        a_wait(k, as_)

        @pl.when(speaks)
        def _():
            b_wait(k, bs)
            b_wait(k, bs)

        @pl.when(jnp.logical_and(p == block - 1, z > 0))
        def _():
            low_down(k).wait_send()

        @pl.when(jnp.logical_and(p == 0, z < blocks - 1))
        def _():
            low_up(k).wait_send()

        @pl.when(me > 0)
        def _():
            drain(hs.at[k, 0], hss.at[k, 0])

        @pl.when(me < n - 1)
        def _():
            drain(hs.at[k, 1], hss.at[k, 1])

    drain(ggat.at[pl.ds(0, n - 1)], gss)
    drain(ggat.at[pl.ds(0, n - 1)], gsr)
    total = jnp.sum(ggat[...], axis=0)
    g01, g11, g02, g12, g22 = (
        jnp.broadcast_to(total[:, j : j + 1], (1, LANES)) for j in range(1, 6)
    )
    ratio = g12 / g11
    c2 = (g02 - ratio * g01) / (g22 - ratio * g12)
    c1 = g01 / g11 - ratio * c2
    coef[0] = jnp.broadcast_to(c1, (8, LANES))
    coef[1] = jnp.broadcast_to(c2, (8, LANES))


def finish(r, u1, u2, w1, w2, coef, x_hbm, res_hbm, xo, ro, x_sem, res_sem):
    layers, rows, depth = r.shape
    step = 8
    c1 = jnp.concatenate([coef[0]] * (depth // LANES), axis=1)
    c2 = jnp.concatenate([coef[1]] * (depth // LANES), axis=1)
    for l in range(layers):
        for y in range(0, rows, step):
            a = PAD + y
            xo[l, y : y + step, :] = (
                c1 * u1[l, a : a + step, :] + c2 * u2[l, a : a + step, :]
            )
        pltpu.make_async_copy(xo.at[l], x_hbm.at[l], x_sem).start()
    for l in range(layers):
        for y in range(0, rows, step):
            ro[l, y : y + step, :] = (
                r[l, y : y + step, :]
                - c1 * w1[l, y : y + step, :] - c2 * w2[l, y : y + step, :]
            )
        pltpu.make_async_copy(ro.at[l], res_hbm.at[l], res_sem).start()
    drain(xo, x_sem)
    drain(ro, res_sem)


def on_device(right_side, sigma, wind, local_inverse, basis_y, basis_z, gamma):
    n = lax.axis_size("sub")
    block = min(8, n)
    blocks = n // block
    layers, rows, depth = right_side.shape
    ky = basis_y.shape[1]
    kz = basis_z.shape[1]
    f32, bf16 = jnp.float32, jnp.bfloat16
    packed = (ky // 2, 2 * kz)
    cube = pltpu.VMEM((layers, rows, depth), f32)
    padded = pltpu.VMEM((layers, rows + 2 * PAD, depth), f32)
    plane = pltpu.VMEM((rows, depth), f32)
    halo = pltpu.VMEM((2, 2, rows, depth), f32)
    dma = pltpu.SemaphoreType.DMA
    scratch = [
        cube, cube,
        pltpu.VMEM((2, rows, depth), f32),
        pltpu.VMEM((1, depth, depth), f32),
        pltpu.VMEM((ky, rows), f32),
        pltpu.VMEM((kz, depth), f32),
        pltpu.VMEM(gamma.shape, f32),
        pltpu.VMEM((depth, depth), bf16),
        pltpu.VMEM((depth, depth), bf16),
        pltpu.VMEM((2 * ky, rows), bf16),
        pltpu.VMEM((rows, 3 * ky), bf16),
        pltpu.VMEM((4 * kz, depth), bf16),
        pltpu.VMEM((6 * kz, depth), bf16),
        pltpu.VMEM((gamma.shape[0],) + packed, f32),
        pltpu.VMEM((rows + 2 * PAD, depth), f32),
        plane, plane, plane,
        pltpu.VMEM((rows, depth), bf16),
        pltpu.VMEM((rows, depth), bf16),
        halo, halo,
        pltpu.VMEM((2,) + packed, f32),
        pltpu.VMEM((2, block) + packed, f32),
        pltpu.VMEM((2,) + packed, f32),
        pltpu.VMEM((2, blocks) + packed, f32),
        pltpu.VMEM((2, 2) + packed, f32),
        pltpu.VMEM((2, 2) + packed, f32),
        pltpu.VMEM((3,) + packed, f32),
        pltpu.VMEM((1, LANES), f32),
        pltpu.VMEM((n, 1, LANES), f32),
        dma((7,)),
        dma((2,)), dma((2,)),
        dma((2,)), dma((2,)),
        dma((2, 2)), dma((2, 2)),
        dma((2, 2)), dma((2, 2, 2)),
        dma, dma,
        pltpu.SemaphoreType.REGULAR((2,)),
        pltpu.SemaphoreType.REGULAR((2, 2)),
    ]
    hbm = pl.BlockSpec(memory_space=pltpu.HBM)
    vmem = pl.BlockSpec(memory_space=pltpu.VMEM)
    out = jax.ShapeDtypeStruct(right_side.shape, f32)
    pieces = pl.pallas_call(
        functools.partial(kernel, n, block),
        out_shape=(cube, padded, padded, cube, cube, pltpu.VMEM((2, 8, LANES), f32)),
        in_specs=[hbm] * 7,
        out_specs=(vmem,) * 6,
        scratch_shapes=scratch,
        compiler_params=pltpu.CompilerParams(
            collective_id=0, has_side_effects=True, vmem_limit_bytes=50 * 2**20,
        ),
        name="gmres",
    )(right_side, sigma, wind, local_inverse, basis_y.T, basis_z.T, gamma)
    return pl.pallas_call(
        finish,
        out_shape=(out, out),
        in_specs=[vmem] * 6,
        out_specs=(hbm, hbm),
        scratch_shapes=[cube, cube, dma, dma],
        compiler_params=pltpu.CompilerParams(vmem_limit_bytes=24 * 2**20),
        name="finish",
    )(*pieces)


def solution(mesh):
    placed = (
        P("sub", None, None),
        P("sub", None, None),
        P("sub", None, None),
        P("sub", None, None),
        P(),
        P(),
        P(),
    )
    return jax.shard_map(
        on_device,
        mesh=mesh,
        in_specs=placed,
        out_specs=(P("sub", None, None), P("sub", None, None)),
        check_vma=False,
    )
```

```python
import functools

import jax
import jax.numpy as jnp
from jax import lax
from jax.experimental import pallas as pl
from jax.experimental.pallas import tpu as pltpu
from jax.sharding import PartitionSpec as P

MESH = pl.DeviceIdType.MESH
PAD = 8
LANES = 128


def split(x):
    hi = x.astype(jnp.bfloat16)
    lo = (x - hi.astype(jnp.float32)).astype(jnp.bfloat16)
    return hi, lo


def mm(a, b):
    return jnp.dot(a, b, preferred_element_type=jnp.float32)


def mt(a, b):
    return lax.dot_general(
        a, b, (((1,), (1,)), ((), ())), preferred_element_type=jnp.float32
    )


def fold(x):
    out = None
    for y in range(0, x.shape[0], 8):
        for at in range(0, x.shape[1], LANES):
            piece = x[y : y + 8, at : at + LANES]
            out = piece if out is None else out + piece
    return out


def flip(i, mask):
    out, bit = i, 1
    while bit <= mask:
        if mask & bit:
            out = out + bit - 2 * bit * lax.rem(lax.div(i, bit), 2)
        bit *= 2
    return out


def drain(ref, sem):
    pltpu.make_async_copy(ref, ref, sem).wait()


def kernel(
    n, block,
    r_hbm, sg_hbm, wd_hbm, li_hbm, by_hbm, bz_hbm, gm_hbm,
    r, u1, u2, w1, w2, coef,
    sw, wde, lf, by, bz, gm, lh, ll, by3, byt, bzp, bz6, fc,
    sp, sb, sa, ys, yh, yl, hs, hr,
    own, gat, tot, allb, low_s, low_r, nbr, gs, ggat,
    in_sem, as_, ar, bs, br, ls, lr, hss, hsr, gss, gsr, ready, go,
):
    layers, rows, depth = r.shape
    ky = by.shape[0]
    half = ky // 2
    kz = bz.shape[0]
    levels = gm.shape[0]
    blocks = n // block
    low_levels = block.bit_length() - 1
    quarter = rows // 8
    spans = (slice(0, quarter), slice(quarter, rows))
    cuts = (0, quarter, 3 * quarter, rows * 11 // 16, rows)
    me = lax.axis_index("sub")
    p = lax.rem(me, block)
    z = lax.div(me, block)
    us = (u1, u2)
    sg, wd = sw.at[0], sw.at[1]
    ws = (w1, w2)
    f32 = jnp.float32

    def load(i, src, dst):
        c = pltpu.make_async_copy(src, dst, in_sem.at[i])
        c.start()
        return c

    c_bz = load(1, bz_hbm, bz)
    c_by = load(2, by_hbm, by)
    c_r = load(0, r_hbm, r)
    c_l = load(3, li_hbm, lf)
    c_gm = load(4, gm_hbm, gm)

    barrier = pltpu.get_barrier_semaphore()
    in_block = [z * block + flip(p, d) for d in range(block - 1, 0, -1)]
    across = [lax.rem(z + d, blocks) * block + p for d in range(1, blocks)]
    beyond = [lax.rem(z + d, blocks) * block + flip(p, 1) for d in range(1, blocks)]
    odd = lax.rem(p, 2) == 1
    even = jnp.logical_not(odd)
    way = lax.rem(p, 2)
    far, near = way * (layers - 1), (1 - way) * (layers - 1)
    speaks = jnp.logical_or(jnp.logical_and(odd, p < block - 1), p == block - 2)
    first_cross = jnp.logical_and(p == 0, z > 0)
    last_cross = jnp.logical_and(p == block - 1, z < blocks - 1)


    def signal(target):
        pl.semaphore_signal(barrier, inc=1, device_id=(target,), device_id_type=MESH)

    for target in in_block + across + beyond:
        signal(target)

    @pl.when(first_cross)
    def _():
        signal(me - 1)

    @pl.when(last_cross)
    def _():
        signal(me + 1)

    zero_rows = jnp.zeros((PAD, depth), f32)
    for u in us:
        for l in range(layers):
            u[l, 0:PAD, :] = zero_rows
            u[l, PAD + rows : PAD + rows + PAD, :] = zero_rows
    sp[0:PAD, :] = zero_rows
    sp[PAD + rows : PAD + rows + PAD, :] = zero_rows

    @pl.when(me == 0)
    def _():
        hr[:, 0] = jnp.zeros((2, rows, depth), f32)

    @pl.when(me == n - 1)
    def _():
        hr[:, 1] = jnp.zeros((2, rows, depth), f32)

    def send(src, dst, s, q, target):
        return pltpu.make_async_remote_copy(
            src_ref=src, dst_ref=dst, send_sem=s, recv_sem=q,
            device_id=(target,), device_id_type=MESH,
        )

    def project(k):
        hi, lo = yh[...], yl[...]
        top = mm(by3[...], hi)
        part = top[0:ky] + top[ky : 2 * ky] + mm(by3[0:ky], lo)
        ph, pl_ = split(part)
        bh, bl = bzp[0 : 2 * kz], bzp[2 * kz : 4 * kz]
        top = mt(jnp.concatenate([ph, pl_], axis=0), bh)
        full = top[0:ky] + top[ky : 2 * ky] + mt(ph, bl)
        lane = lax.broadcasted_iota(jnp.int32, (half, 2 * kz), 1)
        packed = jnp.where(lane < kz, full[0:half], full[half:ky])
        own[k] = packed
        gat[k, p] = packed

    def a_send(k):
        for target in in_block:
            send(own.at[k], gat.at[k, p], as_.at[k], ar.at[k], target).start()
        pl.semaphore_signal(
            ready.at[k], inc=1, device_id=(in_block[-1],), device_id_type=MESH
        )

    def a_wait(k, sem):
        drain(gat.at[k, pl.ds(0, block - 1)], sem.at[k])

    def b_send(k):
        @pl.when(speaks)
        def _():
            for target in across + beyond:
                send(tot.at[k], allb.at[k, z], bs.at[k], br.at[k], target).start()

    def b_wait(k, sem):
        if blocks > 1:
            drain(allb.at[k, pl.ds(0, blocks - 1)], sem.at[k])

    def piece(ref, k, way, at):
        return ref.at[k, way, pl.ds(at.start, at.stop - at.start)]

    def down(k, c, at):
        return send(
            piece(hs, k, 0, at), piece(hr, k, 1, at), hss.at[k, 0], hsr.at[k, 1, c], me - 1
        )

    def up(k, c, at):
        return send(
            piece(hs, k, 1, at), piece(hr, k, 0, at), hss.at[k, 1], hsr.at[k, 0, c], me + 1
        )

    def low_down(k):
        return send(low_s.at[k, 0], low_r.at[k, 1], ls.at[k], lr.at[k], me - block)

    def low_up(k):
        return send(low_s.at[k, 1], low_r.at[k, 0], ls.at[k], lr.at[k], me + block)

    def allow(k, target):
        pl.semaphore_signal(
            go.at[k], inc=1, device_id=(target,), device_id_type=MESH
        )

    def part(i):
        return min(i, 1), slice(cuts[i], cuts[i + 1])

    def cross(k, which):
        @pl.when(first_cross)
        def _():
            if 0 in which:
                pl.semaphore_wait(go.at[k], 1)
            for i in which:
                down(k, *part(i)).start()

        @pl.when(last_cross)
        def _():
            if 0 in which:
                pl.semaphore_wait(go.at[k], 1)
            for i in which:
                up(k, *part(i)).start()

    def times(x):
        xh, xl = split(x)
        m = x.shape[0]
        both = mm(jnp.concatenate([xh, xl], axis=0), lh[...])
        return both[0:m] + both[m : 2 * m] + mm(xh, ll[...])

    def far_edge(k, field, at):
        out = times(field[far, at])
        hs[k, way, at] = out
        us[k][far, PAD + at.start : PAD + at.stop] = out

    def others(k, field):
        inner = range(1, layers - 1)
        out = times(jnp.concatenate([field[near]] + [field[l] for l in inner], axis=0))
        hs[k, 1 - way] = out[0:rows]
        us[k][near, PAD : PAD + rows] = out[0:rows]
        for i, l in enumerate(inner):
            us[k][l, PAD : PAD + rows, :] = out[(i + 1) * rows : (i + 2) * rows]

    def greet(k):
        pl.semaphore_wait(ready.at[k], 1)

        @pl.when(jnp.logical_and(p == block - 1, z > 0))
        def _():
            allow(k, me - block)

        @pl.when(jnp.logical_and(p == 0, z < blocks - 1))
        def _():
            allow(k, me + block)

    def issue(k, which):
        @pl.when(jnp.logical_and(even, p > 0))
        def _():
            for i in which:
                down(k, *part(i)).start()

        @pl.when(jnp.logical_and(odd, p < block - 1))
        def _():
            for i in which:
                up(k, *part(i)).start()

    def issue_near(k):
        @pl.when(even)
        def _():
            for c in range(2):
                up(k, c, spans[c]).start()

        @pl.when(odd)
        def _():
            for c in range(2):
                down(k, c, spans[c]).start()

    def low_part(k, q):
        out = None
        for level in range(low_levels):
            width = 2 ** (level + 1)
            start = lax.div(q, width) * width
            if width == block:
                acc = tot[k]
            else:
                acc = gat[k, start]
                for j in range(1, width):
                    acc = acc + gat[k, start + j]
            term = fc[level] * acc
            out = term if out is None else out + term
        return out

    def high_part(k, zz):
        out = None
        for level in range(low_levels, levels):
            width = 2 ** (level + 1) // block
            start = lax.div(zz, width) * width
            acc = allb[k, start]
            for j in range(1, width):
                acc = acc + allb[k, start + j]
            term = fc[level] * acc
            out = term if out is None else out + term
        return jnp.zeros(tot.shape[1:], f32) if out is None else out

    def exchange(k):
        a_wait(k, ar)
        acc = gat[k, 0]
        for j in range(1, block):
            acc = acc + gat[k, j]
        tot[k] = acc
        allb[k, z] = acc
        b_send(k)

        @pl.when(jnp.logical_and(p == block - 1, z > 0))
        def _():
            low_s[k, 0] = low_part(k, 0)
            low_down(k).start()

        @pl.when(jnp.logical_and(p == 0, z < blocks - 1))
        def _():
            low_s[k, 1] = low_part(k, block - 1)
            low_up(k).start()

        nbr[0] = low_part(k, jnp.maximum(p - 1, 0))
        nbr[1] = low_part(k, p)
        nbr[2] = low_part(k, jnp.minimum(p + 1, block - 1))

        @pl.when(first_cross)
        def _():
            low_up(k).wait_recv()
            nbr[0] = low_r[k, 0]

        @pl.when(last_cross)
        def _():
            low_down(k).wait_recv()
            nbr[2] = low_r[k, 1]

    def back(k):
        b_wait(k, br)
        here = nbr[1] + high_part(k, z)
        before = nbr[0] + high_part(k, lax.div(jnp.maximum(me - 1, 0), block))
        after = nbr[2] + high_part(k, lax.div(jnp.minimum(me + 1, n - 1), block))
        before = jnp.where(me > 0, before, 0.0)
        after = jnp.where(me < n - 1, after, 0.0)
        lane = lax.broadcasted_iota(jnp.int32, (half, 2 * kz), 1)
        three = []
        for c in (here, before, after):
            three += [jnp.where(lane < kz, c, 0.0), jnp.where(lane < kz, 0.0, c)]
        th, tl = split(jnp.concatenate(three, axis=0))
        out = mm(jnp.concatenate([th, tl, th], axis=1), bz6[...])
        th, tl = split(out)
        spreads = []
        for j in range(3):
            piece = slice(j * ky, (j + 1) * ky)
            spreads.append(
                mm(byt[...], jnp.concatenate([th[piece], tl[piece], th[piece]], axis=0))
            )
        sp[PAD : PAD + rows, :] = spreads[0]
        sb[...] = spreads[1]
        sa[...] = spreads[2]

    step = 32

    def beside(ref, l, y):
        a = PAD + y
        here = (lambda s: ref[s, :]) if l is None else (lambda s: ref[l, s, :])
        c = here(slice(a, a + step))
        col = lax.broadcasted_iota(jnp.int32, (step, depth), 1)
        fwd = jnp.where(col == depth - 1, 0.0, pltpu.roll(c, depth - 1, 1))
        bwd = jnp.where(col == 0, 0.0, pltpu.roll(c, 1, 1))
        ups = here(slice(a + 1, a + step + 1))
        downs = here(slice(a - 1, a + step - 1))
        return c, ups + downs + fwd + bwd

    def inner_image(k, which):
        u = us[k]
        for l in which:
            for y in range(0, rows, step):
                a = PAD + y
                at = slice(y, y + step)
                c, around = beside(u, l, y)
                diag = sg[l, at, :] + (4.0 if k == 0 else 0.0)
                out = (2.0 + diag) * c - around
                if k == 0:
                    sg[l, at, :] = diag
                wind = wd[l, at, :]
                if l < layers - 1:
                    out = out + (wind - 1.0) * u[l + 1, a : a + step, :]
                if l > 0:
                    out = out - (wind + 1.0) * u[l - 1, a : a + step, :]
                if k == 0 and l == 0:
                    wde[0, at, :] = wind + 1.0
                if k == 0 and l == layers - 1:
                    wde[1, at, :] = wind - 1.0
                ws[k][l, at, :] = out

    def tally(totals, l, at, out):
        for i, other in enumerate((r, w1, None)):
            other = out if other is None else other[l, at, :]
            term = fold(other * out)
            totals[i] = term if totals[i] is None else totals[i] + term

    outer = (0,) if layers == 1 else (0, layers - 1)

    def image(k, totals):
        w = ws[k]
        for y in range(0, rows, step):
            at = slice(y, y + step)
            s, around = beside(sp, None, y)
            total = None
            for l in range(layers):
                out = w[l, at, :] + (sg[l, at, :] * s - around)
                if l == 0:
                    out = out + wde[0, at, :] * (s - sb[at, :])
                if l == layers - 1:
                    out = out + wde[1, at, :] * (sa[at, :] - s)
                w[l, at, :] = out
                total = out if total is None else total + out
                if k == 1 and l not in outer:
                    tally(totals, l, at, out)
            if k == 0:
                ys[at, :] = total

    def meet(k, c, totals):
        w = ws[k]

        @pl.when(me > 0)
        def _():
            up(k, c, spans[c]).wait_recv()

        @pl.when(me < n - 1)
        def _():
            down(k, c, spans[c]).wait_recv()

        for y in range(spans[c].start, spans[c].stop, quarter):
            at = slice(y, y + quarter)
            change = (-(wde[0, at, :] * hr[k, 0, at, :]), wde[1, at, :] * hr[k, 1, at, :])
            if layers == 1:
                change = (change[0] + change[1],)
            for l, more in zip(outer, change):
                out = w[l, at, :] + more
                w[l, at, :] = out
                if k == 1:
                    tally(totals, l, at, out)
            if k == 0:
                total = ys[at, :]
                for more in change:
                    total = total + more
                yh[at, :], yl[at, :] = split(total)

    def place(totals, first):
        lane = lax.broadcasted_iota(jnp.int32, (8, LANES), 1)
        out = jnp.zeros((8, LANES), f32)
        for i, t in enumerate(totals):
            out = jnp.where(lane == first + i, jnp.sum(t, axis=1, keepdims=True), out)
        return out

    def dots(pairs):
        out = []
        for a, b in pairs:
            acc = None
            for l in range(layers):
                term = fold(a[l] * b[l])
                acc = term if acc is None else acc + term
            out.append(acc)
        return out

    def add_spread(k):
        u = us[k]
        for y in range(0, rows, step):
            s = sp[PAD + y : PAD + y + step, :]
            for l in range(layers):
                u[l, PAD + y : PAD + y + step, :] = u[l, PAD + y : PAD + y + step, :] + s

    c_bz.wait()
    hi, lo = split(bz[...])
    for j in range(2):
        bzp[j * kz : (j + 1) * kz] = hi
        bzp[(2 + j) * kz : (3 + j) * kz] = lo
    for j in range(4):
        bz6[j * kz : (j + 1) * kz] = hi
    for j in range(4, 6):
        bz6[j * kz : (j + 1) * kz] = lo
    c_by.wait()
    hi, lo = split(by[...])
    by3[0:ky] = hi
    by3[ky : 2 * ky] = lo
    c_r.wait()
    for y in range(0, rows, step):
        at = slice(y, y + step)
        total = r[0, at, :]
        for l in range(1, layers):
            total = total + r[l, at, :]
        yh[at, :], yl[at, :] = split(total)
    project(0)
    extra = jnp.where(first_cross, 1, 0) + jnp.where(last_cross, 1, 0)
    pl.semaphore_wait(barrier, block - 1 + 2 * (blocks - 1) + extra)
    a_send(0)
    c_l.wait()
    pltpu.make_async_copy(sg_hbm, sw.at[0], in_sem.at[5]).start()
    pltpu.make_async_copy(wd_hbm, sw.at[1], in_sem.at[5]).start()
    big, small = split(lf[0])
    lh[...] = big
    ll[...] = small
    far_edge(0, r, slice(0, rows))
    greet(0)
    issue(0, (0, 1))
    cross(0, (0, 1))
    others(0, r)
    issue_near(0)
    issue(0, (2,))
    cross(0, (2,))
    c_gm.wait()
    for level in range(levels):
        g = gm[level]
        fc[level] = jnp.concatenate([g[0:half], g[half:ky]], axis=1) * (
            (layers * 2 ** (level + 1)) ** -0.5
        )
    hi, lo = split(by[...].T)
    byt[...] = jnp.concatenate([hi, hi, lo], axis=1)
    drain(sw, in_sem.at[5])
    inner_image(0, range(1))
    issue(0, (3,))
    cross(0, (3,))
    inner_image(0, range(1, layers))
    exchange(0)
    back(0)
    image(0, None)
    meet(0, 0, None)
    far_edge(1, w1, spans[0])
    issue(1, (0,))
    meet(0, 1, None)
    project(1)
    a_send(1)
    far_edge(1, w1, spans[1])
    greet(1)
    issue(1, (1,))
    cross(1, (0, 1))
    others(1, w1)
    issue_near(1)
    issue(1, (2,))
    cross(1, (2,))
    add_spread(0)
    inner_image(1, range(1))
    issue(1, (3,))
    cross(1, (3,))
    inner_image(1, range(1, layers))
    early = place(dots([(r, r), (r, w1), (w1, w1)]), 0)
    exchange(1)
    back(1)
    totals = [None] * 3
    image(1, totals)
    meet(1, 0, totals)
    meet(1, 1, totals)
    late = place(totals, 3)
    flat = jnp.sum(early + late, axis=0, keepdims=True)
    gs[...] = flat
    ggat[me] = flat
    for d in range(n - 1, 0, -1):
        send(gs, ggat.at[me], gss, gsr, flip(me, d)).start()

    add_spread(1)
    for k in range(2):
        a_wait(k, as_)

        @pl.when(speaks)
        def _():
            b_wait(k, bs)
            b_wait(k, bs)

        @pl.when(jnp.logical_and(p == block - 1, z > 0))
        def _():
            low_down(k).wait_send()

        @pl.when(jnp.logical_and(p == 0, z < blocks - 1))
        def _():
            low_up(k).wait_send()

        @pl.when(me > 0)
        def _():
            drain(hs.at[k, 0], hss.at[k, 0])

        @pl.when(me < n - 1)
        def _():
            drain(hs.at[k, 1], hss.at[k, 1])

    drain(ggat.at[pl.ds(0, n - 1)], gss)
    drain(ggat.at[pl.ds(0, n - 1)], gsr)
    total = jnp.sum(ggat[...], axis=0)
    g01, g11, g02, g12, g22 = (
        jnp.broadcast_to(total[:, j : j + 1], (1, LANES)) for j in range(1, 6)
    )
    ratio = g12 / g11
    c2 = (g02 - ratio * g01) / (g22 - ratio * g12)
    c1 = g01 / g11 - ratio * c2
    coef[0] = jnp.broadcast_to(c1, (8, LANES))
    coef[1] = jnp.broadcast_to(c2, (8, LANES))


def finish(r, u1, u2, w1, w2, coef, x_hbm, res_hbm, xo, ro, x_sem, res_sem):
    layers, rows, depth = r.shape
    step, part = 8, 32
    c1 = jnp.concatenate([coef[0]] * (depth // LANES), axis=1)
    c2 = jnp.concatenate([coef[1]] * (depth // LANES), axis=1)

    def flush(buf, out, l, y, sem):
        at = pl.ds(y, part)
        pltpu.make_async_copy(buf.at[l, at], out.at[l, at], sem).start()

    for l in range(layers):
        for y in range(0, rows, step):
            a = PAD + y
            xo[l, y : y + step, :] = (
                c1 * u1[l, a : a + step, :] + c2 * u2[l, a : a + step, :]
            )
            ro[l, y : y + step, :] = (
                r[l, y : y + step, :]
                - c1 * w1[l, y : y + step, :] - c2 * w2[l, y : y + step, :]
            )
            if (y + step) % part == 0:
                flush(xo, x_hbm, l, y + step - part, x_sem)
                flush(ro, res_hbm, l, y + step - part, res_sem)
    drain(xo, x_sem)
    drain(ro, res_sem)


def on_device(right_side, sigma, wind, local_inverse, basis_y, basis_z, gamma):
    n = lax.axis_size("sub")
    block = min(8, n)
    blocks = n // block
    layers, rows, depth = right_side.shape
    ky = basis_y.shape[1]
    kz = basis_z.shape[1]
    f32, bf16 = jnp.float32, jnp.bfloat16
    packed = (ky // 2, 2 * kz)
    cube = pltpu.VMEM((layers, rows, depth), f32)
    padded = pltpu.VMEM((layers, rows + 2 * PAD, depth), f32)
    plane = pltpu.VMEM((rows, depth), f32)
    halo = pltpu.VMEM((2, 2, rows, depth), f32)
    dma = pltpu.SemaphoreType.DMA
    scratch = [
        pltpu.VMEM((2, layers, rows, depth), f32),
        pltpu.VMEM((2, rows, depth), f32),
        pltpu.VMEM((1, depth, depth), f32),
        pltpu.VMEM((ky, rows), f32),
        pltpu.VMEM((kz, depth), f32),
        pltpu.VMEM(gamma.shape, f32),
        pltpu.VMEM((depth, depth), bf16),
        pltpu.VMEM((depth, depth), bf16),
        pltpu.VMEM((2 * ky, rows), bf16),
        pltpu.VMEM((rows, 3 * ky), bf16),
        pltpu.VMEM((4 * kz, depth), bf16),
        pltpu.VMEM((6 * kz, depth), bf16),
        pltpu.VMEM((gamma.shape[0],) + packed, f32),
        pltpu.VMEM((rows + 2 * PAD, depth), f32),
        plane, plane, plane,
        pltpu.VMEM((rows, depth), bf16),
        pltpu.VMEM((rows, depth), bf16),
        halo, halo,
        pltpu.VMEM((2,) + packed, f32),
        pltpu.VMEM((2, block) + packed, f32),
        pltpu.VMEM((2,) + packed, f32),
        pltpu.VMEM((2, blocks) + packed, f32),
        pltpu.VMEM((2, 2) + packed, f32),
        pltpu.VMEM((2, 2) + packed, f32),
        pltpu.VMEM((3,) + packed, f32),
        pltpu.VMEM((1, LANES), f32),
        pltpu.VMEM((n, 1, LANES), f32),
        dma((6,)),
        dma((2,)), dma((2,)),
        dma((2,)), dma((2,)),
        dma((2,)), dma((2,)),
        dma((2, 2)), dma((2, 2, 2)),
        dma, dma,
        pltpu.SemaphoreType.REGULAR((2,)),
        pltpu.SemaphoreType.REGULAR((2,)),
    ]
    hbm = pl.BlockSpec(memory_space=pltpu.HBM)
    vmem = pl.BlockSpec(memory_space=pltpu.VMEM)
    out = jax.ShapeDtypeStruct(right_side.shape, f32)
    pieces = pl.pallas_call(
        functools.partial(kernel, n, block),
        out_shape=(cube, padded, padded, cube, cube, pltpu.VMEM((2, 8, LANES), f32)),
        in_specs=[hbm] * 7,
        out_specs=(vmem,) * 6,
        scratch_shapes=scratch,
        compiler_params=pltpu.CompilerParams(
            collective_id=0, has_side_effects=True, vmem_limit_bytes=50 * 2**20,
        ),
        name="gmres",
    )(right_side, sigma, wind, local_inverse, basis_y.T, basis_z.T, gamma)
    return pl.pallas_call(
        finish,
        out_shape=(out, out),
        in_specs=[vmem] * 6,
        out_specs=(hbm, hbm),
        scratch_shapes=[cube, cube, dma, dma],
        compiler_params=pltpu.CompilerParams(vmem_limit_bytes=24 * 2**20),
        name="finish",
    )(*pieces)


def solution(mesh):
    placed = (
        P("sub", None, None),
        P("sub", None, None),
        P("sub", None, None),
        P("sub", None, None),
        P(),
        P(),
        P(),
    )
    return jax.shard_map(
        on_device,
        mesh=mesh,
        in_specs=placed,
        out_specs=(P("sub", None, None), P("sub", None, None)),
        check_vma=False,
    )
```

```python
import functools

import jax
import jax.numpy as jnp
from jax import lax
from jax.experimental import pallas as pl
from jax.experimental.pallas import tpu as pltpu
from jax.sharding import PartitionSpec as P

MESH = pl.DeviceIdType.MESH
PAD = 8
LANES = 128


def split(x):
    hi = x.astype(jnp.bfloat16)
    lo = (x - hi.astype(jnp.float32)).astype(jnp.bfloat16)
    return hi, lo


def mm(a, b):
    return jnp.dot(a, b, preferred_element_type=jnp.float32)


def mt(a, b):
    return lax.dot_general(
        a, b, (((1,), (1,)), ((), ())), preferred_element_type=jnp.float32
    )


def fold(x):
    out = None
    for y in range(0, x.shape[0], 8):
        for at in range(0, x.shape[1], LANES):
            piece = x[y : y + 8, at : at + LANES]
            out = piece if out is None else out + piece
    return out


def flip(i, mask):
    out, bit = i, 1
    while bit <= mask:
        if mask & bit:
            out = out + bit - 2 * bit * lax.rem(lax.div(i, bit), 2)
        bit *= 2
    return out


def drain(ref, sem):
    pltpu.make_async_copy(ref, ref, sem).wait()


def kernel(
    n, block,
    r_hbm, sg_hbm, wd_hbm, li_hbm, by_hbm, bz_hbm, gm_hbm,
    r, u1, u2, w1, w2, coef,
    sw, wde, lf, by, bz, gm, lh, ll, by3, byt, bzp, bz6, fc,
    sp, sb, sa, ys, yh, yl, hs, hr,
    own, gat, tot, allb, low_s, low_r, nbr, gs, ggat,
    in_sem, out_sem, ar, br, lr, hsr, gsr, ready, go,
):
    layers, rows, depth = r.shape
    ky = by.shape[0]
    half = ky // 2
    kz = bz.shape[0]
    levels = gm.shape[0]
    blocks = n // block
    low_levels = block.bit_length() - 1
    quarter = rows // 4
    spans = (slice(0, quarter), slice(quarter, rows))
    cuts = (0, quarter, 2 * quarter, 3 * quarter, rows)
    me = lax.axis_index("sub")
    p = lax.rem(me, block)
    z = lax.div(me, block)
    us = (u1, u2)
    sg, wd = sw.at[0], sw.at[1]
    ws = (w1, w2)
    f32 = jnp.float32

    def load(i, src, dst):
        c = pltpu.make_async_copy(src, dst, in_sem.at[i])
        c.start()
        return c

    c_bz = load(1, bz_hbm, bz)
    c_by = load(2, by_hbm, by)
    c_r = load(0, r_hbm, r)
    c_l = load(3, li_hbm, lf)
    c_gm = load(4, gm_hbm, gm)

    barrier = pltpu.get_barrier_semaphore()
    in_block = [z * block + flip(p, d) for d in range(block - 1, 0, -1)]
    across = [lax.rem(z + d, blocks) * block + p for d in range(1, blocks)]
    beyond = [lax.rem(z + d, blocks) * block + flip(p, 1) for d in range(1, blocks)]
    odd = lax.rem(p, 2) == 1
    even = jnp.logical_not(odd)
    way = lax.rem(p, 2)
    far, near = way * (layers - 1), (1 - way) * (layers - 1)
    speaks = odd
    first_cross = jnp.logical_and(p == 0, z > 0)
    last_cross = jnp.logical_and(p == block - 1, z < blocks - 1)


    def signal(target):
        pl.semaphore_signal(barrier, inc=1, device_id=(target,), device_id_type=MESH)

    for target in in_block + across + beyond:
        signal(target)

    @pl.when(first_cross)
    def _():
        signal(me - 1)

    @pl.when(last_cross)
    def _():
        signal(me + 1)

    zero_rows = jnp.zeros((PAD, depth), f32)
    for u in us:
        for l in range(layers):
            u[l, 0:PAD, :] = zero_rows
            u[l, PAD + rows : PAD + rows + PAD, :] = zero_rows
    sp[0:PAD, :] = zero_rows
    sp[PAD + rows : PAD + rows + PAD, :] = zero_rows

    @pl.when(me == 0)
    def _():
        hr[:, 0] = jnp.zeros((2, rows, depth), f32)

    @pl.when(me == n - 1)
    def _():
        hr[:, 1] = jnp.zeros((2, rows, depth), f32)

    def send(src, dst, s, q, target):
        return pltpu.make_async_remote_copy(
            src_ref=src, dst_ref=dst, send_sem=s, recv_sem=q,
            device_id=(target,), device_id_type=MESH,
        )

    def project(k):
        hi, lo = yh[...], yl[...]
        top = mm(by3[...], hi)
        part = top[0:ky] + top[ky : 2 * ky] + mm(by3[0:ky], lo)
        ph, pl_ = split(part)
        bh, bl = bzp[0 : 2 * kz], bzp[2 * kz : 4 * kz]
        top = mt(jnp.concatenate([ph, pl_], axis=0), bh)
        full = top[0:ky] + top[ky : 2 * ky] + mt(ph, bl)
        lane = lax.broadcasted_iota(jnp.int32, (half, 2 * kz), 1)
        packed = jnp.where(lane < kz, full[0:half], full[half:ky])
        own[k] = packed
        gat[k, p] = packed

    def a_send(k):
        for target in in_block:
            send(own.at[k], gat.at[k, p], out_sem, ar.at[k], target).start()
        pl.semaphore_signal(
            ready.at[k], inc=1, device_id=(in_block[-1],), device_id_type=MESH
        )

    def a_wait(k, sem):
        drain(gat.at[k, pl.ds(0, block - 1)], sem)

    def b_send(k):
        @pl.when(speaks)
        def _():
            for target in across + beyond:
                send(tot.at[k], allb.at[k, z], out_sem, br.at[k], target).start()

    def b_wait(k, sem):
        if blocks > 1:
            drain(allb.at[k, pl.ds(0, blocks - 1)], sem)

    def piece(ref, k, way, at):
        return ref.at[k, way, pl.ds(at.start, at.stop - at.start)]

    def down(k, c, at):
        return send(
            piece(hs, k, 0, at), piece(hr, k, 1, at), out_sem, hsr.at[k, 1, c], me - 1
        )

    def up(k, c, at):
        return send(
            piece(hs, k, 1, at), piece(hr, k, 0, at), out_sem, hsr.at[k, 0, c], me + 1
        )

    def low_down(k):
        return send(low_s.at[k, 0], low_r.at[k, 1], out_sem, lr.at[k], me - block)

    def low_up(k):
        return send(low_s.at[k, 1], low_r.at[k, 0], out_sem, lr.at[k], me + block)

    def allow(k, target):
        pl.semaphore_signal(
            go.at[k], inc=1, device_id=(target,), device_id_type=MESH
        )

    def part(i):
        return min(i, 1), slice(cuts[i], cuts[i + 1])

    def cross(k, which):
        @pl.when(first_cross)
        def _():
            if 0 in which:
                pl.semaphore_wait(go.at[k], 1)
            for i in which:
                down(k, *part(i)).start()

        @pl.when(last_cross)
        def _():
            if 0 in which:
                pl.semaphore_wait(go.at[k], 1)
            for i in which:
                up(k, *part(i)).start()

    def times(x):
        xh, xl = split(x)
        m = x.shape[0]
        both = mm(jnp.concatenate([xh, xl], axis=0), lh[...])
        return both[0:m] + both[m : 2 * m] + mm(xh, ll[...])

    def far_edge(k, field, at):
        out = times(field[far, at])
        hs[k, way, at] = out
        us[k][far, PAD + at.start : PAD + at.stop] = out

    def others(k, field):
        inner = range(1, layers - 1)
        out = times(jnp.concatenate([field[near]] + [field[l] for l in inner], axis=0))
        hs[k, 1 - way] = out[0:rows]
        us[k][near, PAD : PAD + rows] = out[0:rows]
        for i, l in enumerate(inner):
            us[k][l, PAD : PAD + rows, :] = out[(i + 1) * rows : (i + 2) * rows]

    def greet(k):
        pl.semaphore_wait(ready.at[k], 1)

        @pl.when(jnp.logical_and(p == block - 1, z > 0))
        def _():
            allow(k, me - block)

        @pl.when(jnp.logical_and(p == 0, z < blocks - 1))
        def _():
            allow(k, me + block)

    def issue(k, which):
        @pl.when(jnp.logical_and(even, p > 0))
        def _():
            for i in which:
                down(k, *part(i)).start()

        @pl.when(jnp.logical_and(odd, p < block - 1))
        def _():
            for i in which:
                up(k, *part(i)).start()

    def issue_near(k):
        @pl.when(even)
        def _():
            for c in range(2):
                up(k, c, spans[c]).start()

        @pl.when(odd)
        def _():
            for c in range(2):
                down(k, c, spans[c]).start()

    def low_part(k, q):
        out = None
        for level in range(low_levels):
            width = 2 ** (level + 1)
            start = lax.div(q, width) * width
            if width == block:
                acc = tot[k]
            else:
                acc = gat[k, start]
                for j in range(1, width):
                    acc = acc + gat[k, start + j]
            term = fc[level] * acc
            out = term if out is None else out + term
        return out

    def high_part(k, zz):
        out = None
        for level in range(low_levels, levels):
            width = 2 ** (level + 1) // block
            start = lax.div(zz, width) * width
            acc = allb[k, start]
            for j in range(1, width):
                acc = acc + allb[k, start + j]
            term = fc[level] * acc
            out = term if out is None else out + term
        return jnp.zeros(tot.shape[1:], f32) if out is None else out

    def exchange(k):
        a_wait(k, ar.at[k])
        acc = gat[k, 0]
        for j in range(1, block):
            acc = acc + gat[k, j]
        tot[k] = acc
        allb[k, z] = acc
        b_send(k)

        @pl.when(jnp.logical_and(p == block - 1, z > 0))
        def _():
            low_s[k, 0] = low_part(k, 0)
            low_down(k).start()

        @pl.when(jnp.logical_and(p == 0, z < blocks - 1))
        def _():
            low_s[k, 1] = low_part(k, block - 1)
            low_up(k).start()

        nbr[0] = low_part(k, jnp.maximum(p - 1, 0))
        nbr[1] = low_part(k, p)
        nbr[2] = low_part(k, jnp.minimum(p + 1, block - 1))

        @pl.when(first_cross)
        def _():
            low_up(k).wait_recv()
            nbr[0] = low_r[k, 0]

        @pl.when(last_cross)
        def _():
            low_down(k).wait_recv()
            nbr[2] = low_r[k, 1]

    def back(k):
        b_wait(k, br.at[k])
        here = nbr[1] + high_part(k, z)
        before = nbr[0] + high_part(k, lax.div(jnp.maximum(me - 1, 0), block))
        after = nbr[2] + high_part(k, lax.div(jnp.minimum(me + 1, n - 1), block))
        before = jnp.where(me > 0, before, 0.0)
        after = jnp.where(me < n - 1, after, 0.0)
        lane = lax.broadcasted_iota(jnp.int32, (half, 2 * kz), 1)
        three = []
        for c in (here, before, after):
            three += [jnp.where(lane < kz, c, 0.0), jnp.where(lane < kz, 0.0, c)]
        th, tl = split(jnp.concatenate(three, axis=0))
        out = mm(jnp.concatenate([th, tl, th], axis=1), bz6[...])
        th, tl = split(out)
        spreads = []
        for j in range(3):
            piece = slice(j * ky, (j + 1) * ky)
            spreads.append(
                mm(byt[...], jnp.concatenate([th[piece], tl[piece], th[piece]], axis=0))
            )
        sp[PAD : PAD + rows, :] = spreads[0]
        sb[...] = spreads[1]
        sa[...] = spreads[2]

    step = 32

    def beside(ref, l, y):
        a = PAD + y
        here = (lambda s: ref[s, :]) if l is None else (lambda s: ref[l, s, :])
        c = here(slice(a, a + step))
        col = lax.broadcasted_iota(jnp.int32, (step, depth), 1)
        fwd = jnp.where(col == depth - 1, 0.0, pltpu.roll(c, depth - 1, 1))
        bwd = jnp.where(col == 0, 0.0, pltpu.roll(c, 1, 1))
        ups = here(slice(a + 1, a + step + 1))
        downs = here(slice(a - 1, a + step - 1))
        return c, ups + downs + fwd + bwd

    def inner_image(k, which):
        u = us[k]
        for l in which:
            for y in range(0, rows, step):
                a = PAD + y
                at = slice(y, y + step)
                c, around = beside(u, l, y)
                diag = sg[l, at, :] + (4.0 if k == 0 else 0.0)
                out = (2.0 + diag) * c - around
                if k == 0:
                    sg[l, at, :] = diag
                wind = wd[l, at, :]
                if l < layers - 1:
                    out = out + (wind - 1.0) * u[l + 1, a : a + step, :]
                if l > 0:
                    out = out - (wind + 1.0) * u[l - 1, a : a + step, :]
                if k == 0 and l == 0:
                    wde[0, at, :] = wind + 1.0
                if k == 0 and l == layers - 1:
                    wde[1, at, :] = wind - 1.0
                ws[k][l, at, :] = out

    def tally(totals, l, at, out):
        for i, other in enumerate((r, w1, None)):
            other = out if other is None else other[l, at, :]
            term = fold(other * out)
            totals[i] = term if totals[i] is None else totals[i] + term

    outer = (0,) if layers == 1 else (0, layers - 1)

    def image(k, totals):
        w = ws[k]
        for y in range(0, rows, step):
            at = slice(y, y + step)
            s, around = beside(sp, None, y)
            total = None
            for l in range(layers):
                out = w[l, at, :] + (sg[l, at, :] * s - around)
                if l == 0:
                    out = out + wde[0, at, :] * (s - sb[at, :])
                if l == layers - 1:
                    out = out + wde[1, at, :] * (sa[at, :] - s)
                w[l, at, :] = out
                total = out if total is None else total + out
                if k == 1 and l not in outer:
                    tally(totals, l, at, out)
            if k == 0:
                ys[at, :] = total

    def meet(k, c, totals):
        w = ws[k]

        @pl.when(me > 0)
        def _():
            up(k, c, spans[c]).wait_recv()

        @pl.when(me < n - 1)
        def _():
            down(k, c, spans[c]).wait_recv()

        for y in range(spans[c].start, spans[c].stop, quarter):
            at = slice(y, y + quarter)
            change = (-(wde[0, at, :] * hr[k, 0, at, :]), wde[1, at, :] * hr[k, 1, at, :])
            if layers == 1:
                change = (change[0] + change[1],)
            for l, more in zip(outer, change):
                out = w[l, at, :] + more
                w[l, at, :] = out
                if k == 1:
                    tally(totals, l, at, out)
            if k == 0:
                total = ys[at, :]
                for more in change:
                    total = total + more
                yh[at, :], yl[at, :] = split(total)

    def place(totals, first):
        lane = lax.broadcasted_iota(jnp.int32, (8, LANES), 1)
        out = jnp.zeros((8, LANES), f32)
        for i, t in enumerate(totals):
            out = jnp.where(lane == first + i, jnp.sum(t, axis=1, keepdims=True), out)
        return out

    def dots(pairs):
        out = []
        for a, b in pairs:
            acc = None
            for l in range(layers):
                term = fold(a[l] * b[l])
                acc = term if acc is None else acc + term
            out.append(acc)
        return out

    def add_spread(k):
        u = us[k]
        for y in range(0, rows, step):
            s = sp[PAD + y : PAD + y + step, :]
            for l in range(layers):
                u[l, PAD + y : PAD + y + step, :] = u[l, PAD + y : PAD + y + step, :] + s

    c_bz.wait()
    hi, lo = split(bz[...])
    for j in range(2):
        bzp[j * kz : (j + 1) * kz] = hi
        bzp[(2 + j) * kz : (3 + j) * kz] = lo
    c_by.wait()
    hi, lo = split(by[...])
    by3[0:ky] = hi
    by3[ky : 2 * ky] = lo
    c_r.wait()
    for y in range(0, rows, step):
        at = slice(y, y + step)
        total = r[0, at, :]
        for l in range(1, layers):
            total = total + r[l, at, :]
        yh[at, :], yl[at, :] = split(total)
    project(0)
    extra = jnp.where(first_cross, 1, 0) + jnp.where(last_cross, 1, 0)
    pl.semaphore_wait(barrier, block - 1 + 2 * (blocks - 1) + extra)
    a_send(0)
    c_l.wait()
    pltpu.make_async_copy(sg_hbm, sw.at[0], in_sem.at[5]).start()
    pltpu.make_async_copy(wd_hbm, sw.at[1], in_sem.at[5]).start()
    big, small = split(lf[0])
    lh[...] = big
    ll[...] = small
    far_edge(0, r, slice(0, rows))
    greet(0)
    issue(0, (0, 1))
    cross(0, (0, 1))
    others(0, r)
    issue_near(0)
    issue(0, (2,))
    cross(0, (2,))
    c_gm.wait()
    for level in range(levels):
        g = gm[level]
        fc[level] = jnp.concatenate([g[0:half], g[half:ky]], axis=1) * (
            (layers * 2 ** (level + 1)) ** -0.5
        )
    for j in range(2):
        bz6[2 * j * kz : (2 * j + 2) * kz] = bzp[0 : 2 * kz]
    bz6[4 * kz : 6 * kz] = bzp[2 * kz : 4 * kz]
    hi, lo = split(by[...].T)
    byt[...] = jnp.concatenate([hi, hi, lo], axis=1)
    drain(sw, in_sem.at[5])
    inner_image(0, range(1))
    issue(0, (3,))
    cross(0, (3,))
    inner_image(0, range(1, layers))
    exchange(0)
    back(0)
    image(0, None)
    meet(0, 0, None)
    far_edge(1, w1, spans[0])
    issue(1, (0,))
    meet(0, 1, None)
    project(1)
    a_send(1)
    far_edge(1, w1, spans[1])
    greet(1)
    issue(1, (1,))
    cross(1, (0, 1))
    others(1, w1)
    issue_near(1)
    issue(1, (2,))
    cross(1, (2,))
    add_spread(0)
    inner_image(1, range(1))
    issue(1, (3,))
    cross(1, (3,))
    inner_image(1, range(1, layers))
    early = place(dots([(r, r), (r, w1), (w1, w1)]), 0)
    exchange(1)
    back(1)
    totals = [None] * 3
    image(1, totals)
    meet(1, 0, totals)
    meet(1, 1, totals)
    late = place(totals, 3)
    flat = jnp.sum(early + late, axis=0, keepdims=True)
    gs[...] = flat
    ggat[me] = flat
    for d in range(n - 1, 0, -1):
        send(gs, ggat.at[me], out_sem, gsr, flip(me, d)).start()

    add_spread(1)
    for k in range(2):
        a_wait(k, out_sem)

        @pl.when(speaks)
        def _():
            b_wait(k, out_sem)
            b_wait(k, out_sem)

        @pl.when(jnp.logical_and(p == block - 1, z > 0))
        def _():
            low_down(k).wait_send()

        @pl.when(jnp.logical_and(p == 0, z < blocks - 1))
        def _():
            low_up(k).wait_send()

        @pl.when(me > 0)
        def _():
            drain(hs.at[k, 0], out_sem)

        @pl.when(me < n - 1)
        def _():
            drain(hs.at[k, 1], out_sem)

    drain(ggat.at[pl.ds(0, n - 1)], out_sem)
    drain(ggat.at[pl.ds(0, n - 1)], gsr)
    total = jnp.sum(ggat[...], axis=0)
    g01, g11, g02, g12, g22 = (
        jnp.broadcast_to(total[:, j : j + 1], (1, LANES)) for j in range(1, 6)
    )
    ratio = g12 / g11
    c2 = (g02 - ratio * g01) / (g22 - ratio * g12)
    c1 = g01 / g11 - ratio * c2
    coef[0] = jnp.broadcast_to(c1, (8, LANES))
    coef[1] = jnp.broadcast_to(c2, (8, LANES))


def finish(r, u1, u2, w1, w2, coef, x_hbm, res_hbm, xo, ro, x_sem, res_sem):
    layers, rows, depth = r.shape
    step, part = 8, 32
    c1 = jnp.concatenate([coef[0]] * (depth // LANES), axis=1)
    c2 = jnp.concatenate([coef[1]] * (depth // LANES), axis=1)

    def flush(buf, out, l, y, sem):
        at = pl.ds(y, part)
        pltpu.make_async_copy(buf.at[l, at], out.at[l, at], sem).start()

    for l in range(layers):
        for y in range(0, rows, step):
            a = PAD + y
            xo[l, y : y + step, :] = (
                c1 * u1[l, a : a + step, :] + c2 * u2[l, a : a + step, :]
            )
            ro[l, y : y + step, :] = (
                r[l, y : y + step, :]
                - c1 * w1[l, y : y + step, :] - c2 * w2[l, y : y + step, :]
            )
            if (y + step) % part == 0:
                flush(xo, x_hbm, l, y + step - part, x_sem)
                flush(ro, res_hbm, l, y + step - part, res_sem)
    drain(xo, x_sem)
    drain(ro, res_sem)


def on_device(right_side, sigma, wind, local_inverse, basis_y, basis_z, gamma):
    n = lax.axis_size("sub")
    block = min(8, n)
    blocks = n // block
    layers, rows, depth = right_side.shape
    ky = basis_y.shape[1]
    kz = basis_z.shape[1]
    f32, bf16 = jnp.float32, jnp.bfloat16
    packed = (ky // 2, 2 * kz)
    cube = pltpu.VMEM((layers, rows, depth), f32)
    padded = pltpu.VMEM((layers, rows + 2 * PAD, depth), f32)
    plane = pltpu.VMEM((rows, depth), f32)
    halo = pltpu.VMEM((2, 2, rows, depth), f32)
    dma = pltpu.SemaphoreType.DMA
    scratch = [
        pltpu.VMEM((2, layers, rows, depth), f32),
        pltpu.VMEM((2, rows, depth), f32),
        pltpu.VMEM((1, depth, depth), f32),
        pltpu.VMEM((ky, rows), f32),
        pltpu.VMEM((kz, depth), f32),
        pltpu.VMEM(gamma.shape, f32),
        pltpu.VMEM((depth, depth), bf16),
        pltpu.VMEM((depth, depth), bf16),
        pltpu.VMEM((2 * ky, rows), bf16),
        pltpu.VMEM((rows, 3 * ky), bf16),
        pltpu.VMEM((4 * kz, depth), bf16),
        pltpu.VMEM((6 * kz, depth), bf16),
        pltpu.VMEM((gamma.shape[0],) + packed, f32),
        pltpu.VMEM((rows + 2 * PAD, depth), f32),
        plane, plane, plane,
        pltpu.VMEM((rows, depth), bf16),
        pltpu.VMEM((rows, depth), bf16),
        halo, halo,
        pltpu.VMEM((2,) + packed, f32),
        pltpu.VMEM((2, block) + packed, f32),
        pltpu.VMEM((2,) + packed, f32),
        pltpu.VMEM((2, blocks) + packed, f32),
        pltpu.VMEM((2, 2) + packed, f32),
        pltpu.VMEM((2, 2) + packed, f32),
        pltpu.VMEM((3,) + packed, f32),
        pltpu.VMEM((1, LANES), f32),
        pltpu.VMEM((n, 1, LANES), f32),
        dma((6,)), dma,
        dma((2,)), dma((2,)), dma((2,)), dma((2, 2, 2)),
        dma,
        pltpu.SemaphoreType.REGULAR((2,)),
        pltpu.SemaphoreType.REGULAR((2,)),
    ]
    hbm = pl.BlockSpec(memory_space=pltpu.HBM)
    vmem = pl.BlockSpec(memory_space=pltpu.VMEM)
    out = jax.ShapeDtypeStruct(right_side.shape, f32)
    pieces = pl.pallas_call(
        functools.partial(kernel, n, block),
        out_shape=(cube, padded, padded, cube, cube, pltpu.VMEM((2, 8, LANES), f32)),
        in_specs=[hbm] * 7,
        out_specs=(vmem,) * 6,
        scratch_shapes=scratch,
        compiler_params=pltpu.CompilerParams(
            collective_id=0, has_side_effects=True, vmem_limit_bytes=50 * 2**20,
        ),
        name="gmres",
    )(right_side, sigma, wind, local_inverse, basis_y.T, basis_z.T, gamma)
    return pl.pallas_call(
        finish,
        out_shape=(out, out),
        in_specs=[vmem] * 6,
        out_specs=(hbm, hbm),
        scratch_shapes=[cube, cube, dma, dma],
        compiler_params=pltpu.CompilerParams(vmem_limit_bytes=24 * 2**20),
        name="finish",
    )(*pieces)


def solution(mesh):
    placed = (
        P("sub", None, None),
        P("sub", None, None),
        P("sub", None, None),
        P("sub", None, None),
        P(),
        P(),
        P(),
    )
    return jax.shard_map(
        on_device,
        mesh=mesh,
        in_specs=placed,
        out_specs=(P("sub", None, None), P("sub", None, None)),
        check_vma=False,
    )
```

```python
import functools

import jax
import jax.numpy as jnp
from jax import lax
from jax.experimental import pallas as pl
from jax.experimental.pallas import tpu as pltpu
from jax.sharding import PartitionSpec as P

MESH = pl.DeviceIdType.MESH
PAD = 8
LANES = 128


def split(x):
    hi = x.astype(jnp.bfloat16)
    lo = (x - hi.astype(jnp.float32)).astype(jnp.bfloat16)
    return hi, lo


def mm(a, b):
    return jnp.dot(a, b, preferred_element_type=jnp.float32)


def mt(a, b):
    return lax.dot_general(
        a, b, (((1,), (1,)), ((), ())), preferred_element_type=jnp.float32
    )


def fold(x):
    out = None
    for y in range(0, x.shape[0], 8):
        for at in range(0, x.shape[1], LANES):
            piece = x[y : y + 8, at : at + LANES]
            out = piece if out is None else out + piece
    return out


def flip(i, mask):
    out, bit = i, 1
    while bit <= mask:
        if mask & bit:
            out = out + bit - 2 * bit * lax.rem(lax.div(i, bit), 2)
        bit *= 2
    return out


def drain(ref, sem):
    pltpu.make_async_copy(ref, ref, sem).wait()


def kernel(
    n, block,
    r_hbm, sg_hbm, wd_hbm, li_hbm, by_hbm, bz_hbm, gm_hbm,
    r, u1, u2, w1, w2, coef,
    sw, wde, lf, by, bz, gm, lh, ll, by3, byt, bzp, bz6, fc,
    sp, sb, sa, ys, yh, yl, hs, hr,
    own, gat, tot, allb, low_s, low_r, nbr, gs, ggat,
    in_sem, out_sem, ar, br, lr, hsr, gsr, ready, go,
):
    layers, rows, depth = r.shape
    ky = by.shape[0]
    half = ky // 2
    kz = bz.shape[0]
    levels = gm.shape[0]
    blocks = n // block
    low_levels = block.bit_length() - 1
    quarter = rows // 4
    spans = (slice(0, quarter), slice(quarter, rows))
    cuts = (0, quarter, 2 * quarter, 3 * quarter, rows)
    me = lax.axis_index("sub")
    p = lax.rem(me, block)
    z = lax.div(me, block)
    us = (u1, u2)
    sg, wd = sw.at[0], sw.at[1]
    ws = (w1, w2)
    f32 = jnp.float32

    def load(i, src, dst):
        c = pltpu.make_async_copy(src, dst, in_sem.at[i])
        c.start()
        return c

    c_bz = load(1, bz_hbm, bz)
    c_by = load(2, by_hbm, by)
    c_r = load(0, r_hbm, r)

    barrier = pltpu.get_barrier_semaphore()
    in_block = [z * block + flip(p, d) for d in range(block - 1, 0, -1)]
    across = [lax.rem(z + d, blocks) * block + p for d in range(1, blocks)]
    beyond = [lax.rem(z + d, blocks) * block + flip(p, 1) for d in range(1, blocks)]
    odd = lax.rem(p, 2) == 1
    even = jnp.logical_not(odd)
    way = lax.rem(p, 2)
    far, near = way * (layers - 1), (1 - way) * (layers - 1)
    speaks = odd
    first_cross = jnp.logical_and(p == 0, z > 0)
    last_cross = jnp.logical_and(p == block - 1, z < blocks - 1)


    def signal(target):
        pl.semaphore_signal(barrier, inc=1, device_id=(target,), device_id_type=MESH)

    for target in in_block + across + beyond:
        signal(target)

    @pl.when(first_cross)
    def _():
        signal(me - 1)

    @pl.when(last_cross)
    def _():
        signal(me + 1)

    zero_rows = jnp.zeros((PAD, depth), f32)
    for u in us:
        for l in range(layers):
            u[l, 0:PAD, :] = zero_rows
            u[l, PAD + rows : PAD + rows + PAD, :] = zero_rows
    sp[0:PAD, :] = zero_rows
    sp[PAD + rows : PAD + rows + PAD, :] = zero_rows

    @pl.when(me == 0)
    def _():
        hr[:, 0] = jnp.zeros((2, rows, depth), f32)

    @pl.when(me == n - 1)
    def _():
        hr[:, 1] = jnp.zeros((2, rows, depth), f32)

    def send(src, dst, s, q, target):
        return pltpu.make_async_remote_copy(
            src_ref=src, dst_ref=dst, send_sem=s, recv_sem=q,
            device_id=(target,), device_id_type=MESH,
        )

    def project(k):
        hi, lo = yh[...], yl[...]
        top = mm(by3[...], hi)
        part = top[0:ky] + top[ky : 2 * ky] + mm(by3[0:ky], lo)
        ph, pl_ = split(part)
        bh, bl = bzp[0 : 2 * kz], bzp[2 * kz : 4 * kz]
        top = mt(jnp.concatenate([ph, pl_], axis=0), bh)
        full = top[0:ky] + top[ky : 2 * ky] + mt(ph, bl)
        lane = lax.broadcasted_iota(jnp.int32, (half, 2 * kz), 1)
        packed = jnp.where(lane < kz, full[0:half], full[half:ky])
        own[k] = packed
        gat[k, p] = packed

    def a_send(k):
        for target in in_block:
            send(own.at[k], gat.at[k, p], out_sem, ar.at[k], target).start()
        pl.semaphore_signal(
            ready.at[k], inc=1, device_id=(in_block[-1],), device_id_type=MESH
        )

    def a_wait(k, sem):
        drain(gat.at[k, pl.ds(0, block - 1)], sem)

    def b_send(k):
        @pl.when(speaks)
        def _():
            for target in across + beyond:
                send(tot.at[k], allb.at[k, z], out_sem, br.at[k], target).start()

    def b_wait(k, sem):
        if blocks > 1:
            drain(allb.at[k, pl.ds(0, blocks - 1)], sem)

    def piece(ref, k, way, at):
        return ref.at[k, way, pl.ds(at.start, at.stop - at.start)]

    def down(k, c, at):
        return send(
            piece(hs, k, 0, at), piece(hr, k, 1, at), out_sem, hsr.at[k, 1, c], me - 1
        )

    def up(k, c, at):
        return send(
            piece(hs, k, 1, at), piece(hr, k, 0, at), out_sem, hsr.at[k, 0, c], me + 1
        )

    def low_down(k):
        return send(low_s.at[k, 0], low_r.at[k, 1], out_sem, lr.at[k], me - block)

    def low_up(k):
        return send(low_s.at[k, 1], low_r.at[k, 0], out_sem, lr.at[k], me + block)

    def allow(k, target):
        pl.semaphore_signal(
            go.at[k], inc=1, device_id=(target,), device_id_type=MESH
        )

    def part(i):
        return min(i, 1), slice(cuts[i], cuts[i + 1])

    def cross(k, which):
        @pl.when(first_cross)
        def _():
            if 0 in which:
                pl.semaphore_wait(go.at[k], 1)
            for i in which:
                down(k, *part(i)).start()

        @pl.when(last_cross)
        def _():
            if 0 in which:
                pl.semaphore_wait(go.at[k], 1)
            for i in which:
                up(k, *part(i)).start()

    def times(x):
        xh, xl = split(x)
        m = x.shape[0]
        both = mm(jnp.concatenate([xh, xl], axis=0), lh[...])
        return both[0:m] + both[m : 2 * m] + mm(xh, ll[...])

    def far_edge(k, field, at):
        out = times(field[far, at])
        hs[k, way, at] = out
        us[k][far, PAD + at.start : PAD + at.stop] = out

    def others(k, field):
        inner = range(1, layers - 1)
        out = times(jnp.concatenate([field[near]] + [field[l] for l in inner], axis=0))
        hs[k, 1 - way] = out[0:rows]
        us[k][near, PAD : PAD + rows] = out[0:rows]
        for i, l in enumerate(inner):
            us[k][l, PAD : PAD + rows, :] = out[(i + 1) * rows : (i + 2) * rows]

    def greet(k):
        pl.semaphore_wait(ready.at[k], 1)

        @pl.when(jnp.logical_and(p == block - 1, z > 0))
        def _():
            allow(k, me - block)

        @pl.when(jnp.logical_and(p == 0, z < blocks - 1))
        def _():
            allow(k, me + block)

    def issue(k, which):
        @pl.when(jnp.logical_and(even, p > 0))
        def _():
            for i in which:
                down(k, *part(i)).start()

        @pl.when(jnp.logical_and(odd, p < block - 1))
        def _():
            for i in which:
                up(k, *part(i)).start()

    def issue_near(k):
        @pl.when(even)
        def _():
            for c in range(2):
                up(k, c, spans[c]).start()

        @pl.when(odd)
        def _():
            for c in range(2):
                down(k, c, spans[c]).start()

    def low_part(k, q):
        out = None
        for level in range(low_levels):
            width = 2 ** (level + 1)
            start = lax.div(q, width) * width
            if width == block:
                acc = tot[k]
            else:
                acc = gat[k, start]
                for j in range(1, width):
                    acc = acc + gat[k, start + j]
            term = fc[level] * acc
            out = term if out is None else out + term
        return out

    def high_part(k, zz):
        out = None
        for level in range(low_levels, levels):
            width = 2 ** (level + 1) // block
            start = lax.div(zz, width) * width
            acc = allb[k, start]
            for j in range(1, width):
                acc = acc + allb[k, start + j]
            term = fc[level] * acc
            out = term if out is None else out + term
        return jnp.zeros(tot.shape[1:], f32) if out is None else out

    def exchange(k):
        a_wait(k, ar.at[k])
        acc = gat[k, 0]
        for j in range(1, block):
            acc = acc + gat[k, j]
        tot[k] = acc
        allb[k, z] = acc
        b_send(k)

        @pl.when(jnp.logical_and(p == block - 1, z > 0))
        def _():
            low_s[k, 0] = low_part(k, 0)
            low_down(k).start()

        @pl.when(jnp.logical_and(p == 0, z < blocks - 1))
        def _():
            low_s[k, 1] = low_part(k, block - 1)
            low_up(k).start()

        nbr[0] = low_part(k, jnp.maximum(p - 1, 0))
        nbr[1] = low_part(k, p)
        nbr[2] = low_part(k, jnp.minimum(p + 1, block - 1))

        @pl.when(first_cross)
        def _():
            low_up(k).wait_recv()
            nbr[0] = low_r[k, 0]

        @pl.when(last_cross)
        def _():
            low_down(k).wait_recv()
            nbr[2] = low_r[k, 1]

    def back(k):
        b_wait(k, br.at[k])
        here = nbr[1] + high_part(k, z)
        before = nbr[0] + high_part(k, lax.div(jnp.maximum(me - 1, 0), block))
        after = nbr[2] + high_part(k, lax.div(jnp.minimum(me + 1, n - 1), block))
        before = jnp.where(me > 0, before, 0.0)
        after = jnp.where(me < n - 1, after, 0.0)
        lane = lax.broadcasted_iota(jnp.int32, (half, 2 * kz), 1)
        three = []
        for c in (here, before, after):
            three += [jnp.where(lane < kz, c, 0.0), jnp.where(lane < kz, 0.0, c)]
        th, tl = split(jnp.concatenate(three, axis=0))
        out = mm(jnp.concatenate([th, tl, th], axis=1), bz6[...])
        th, tl = split(out)
        spreads = []
        for j in range(3):
            piece = slice(j * ky, (j + 1) * ky)
            spreads.append(
                mm(byt[...], jnp.concatenate([th[piece], tl[piece], th[piece]], axis=0))
            )
        sp[PAD : PAD + rows, :] = spreads[0]
        sb[...] = spreads[1]
        sa[...] = spreads[2]

    step = 32

    def beside(ref, l, y):
        a = PAD + y
        here = (lambda s: ref[s, :]) if l is None else (lambda s: ref[l, s, :])
        c = here(slice(a, a + step))
        col = lax.broadcasted_iota(jnp.int32, (step, depth), 1)
        fwd = jnp.where(col == depth - 1, 0.0, pltpu.roll(c, depth - 1, 1))
        bwd = jnp.where(col == 0, 0.0, pltpu.roll(c, 1, 1))
        ups = here(slice(a + 1, a + step + 1))
        downs = here(slice(a - 1, a + step - 1))
        return c, ups + downs + fwd + bwd

    def inner_image(k, which):
        u = us[k]
        for l in which:
            for y in range(0, rows, step):
                a = PAD + y
                at = slice(y, y + step)
                c, around = beside(u, l, y)
                diag = sg[l, at, :] + (4.0 if k == 0 else 0.0)
                out = (2.0 + diag) * c - around
                if k == 0:
                    sg[l, at, :] = diag
                wind = wd[l, at, :]
                if l < layers - 1:
                    out = out + (wind - 1.0) * u[l + 1, a : a + step, :]
                if l > 0:
                    out = out - (wind + 1.0) * u[l - 1, a : a + step, :]
                if k == 0 and l == 0:
                    wde[0, at, :] = wind + 1.0
                if k == 0 and l == layers - 1:
                    wde[1, at, :] = wind - 1.0
                ws[k][l, at, :] = out

    def tally(totals, l, at, out):
        for i, other in enumerate((r, w1, None)):
            other = out if other is None else other[l, at, :]
            term = fold(other * out)
            totals[i] = term if totals[i] is None else totals[i] + term

    outer = (0,) if layers == 1 else (0, layers - 1)

    def image(k, totals):
        w = ws[k]
        for y in range(0, rows, step):
            at = slice(y, y + step)
            s, around = beside(sp, None, y)
            total = None
            for l in range(layers):
                out = w[l, at, :] + (sg[l, at, :] * s - around)
                if l == 0:
                    out = out + wde[0, at, :] * (s - sb[at, :])
                if l == layers - 1:
                    out = out + wde[1, at, :] * (sa[at, :] - s)
                w[l, at, :] = out
                total = out if total is None else total + out
                if k == 1 and l not in outer:
                    tally(totals, l, at, out)
            if k == 0:
                ys[at, :] = total

    def meet(k, c, totals):
        w = ws[k]

        @pl.when(me > 0)
        def _():
            up(k, c, spans[c]).wait_recv()

        @pl.when(me < n - 1)
        def _():
            down(k, c, spans[c]).wait_recv()

        for y in range(spans[c].start, spans[c].stop, quarter):
            at = slice(y, y + quarter)
            change = (-(wde[0, at, :] * hr[k, 0, at, :]), wde[1, at, :] * hr[k, 1, at, :])
            if layers == 1:
                change = (change[0] + change[1],)
            for l, more in zip(outer, change):
                out = w[l, at, :] + more
                w[l, at, :] = out
                if k == 1:
                    tally(totals, l, at, out)
            if k == 0:
                total = ys[at, :]
                for more in change:
                    total = total + more
                yh[at, :], yl[at, :] = split(total)

    def place(totals, first):
        lane = lax.broadcasted_iota(jnp.int32, (8, LANES), 1)
        out = jnp.zeros((8, LANES), f32)
        for i, t in enumerate(totals):
            out = jnp.where(lane == first + i, jnp.sum(t, axis=1, keepdims=True), out)
        return out

    def dots(pairs):
        out = []
        for a, b in pairs:
            acc = None
            for l in range(layers):
                term = fold(a[l] * b[l])
                acc = term if acc is None else acc + term
            out.append(acc)
        return out

    def add_spread(k):
        u = us[k]
        for y in range(0, rows, step):
            s = sp[PAD + y : PAD + y + step, :]
            for l in range(layers):
                u[l, PAD + y : PAD + y + step, :] = u[l, PAD + y : PAD + y + step, :] + s

    c_bz.wait()
    c_l = load(3, li_hbm, lf)
    c_gm = load(4, gm_hbm, gm)
    hi, lo = split(bz[...])
    for j in range(2):
        bzp[j * kz : (j + 1) * kz] = hi
        bzp[(2 + j) * kz : (3 + j) * kz] = lo
    c_by.wait()
    hi, lo = split(by[...])
    by3[0:ky] = hi
    by3[ky : 2 * ky] = lo
    c_r.wait()
    for y in range(0, rows, step):
        at = slice(y, y + step)
        total = r[0, at, :]
        for l in range(1, layers):
            total = total + r[l, at, :]
        yh[at, :], yl[at, :] = split(total)
    project(0)
    extra = jnp.where(first_cross, 1, 0) + jnp.where(last_cross, 1, 0)
    pl.semaphore_wait(barrier, block - 1 + 2 * (blocks - 1) + extra)
    a_send(0)
    c_l.wait()
    pltpu.make_async_copy(sg_hbm, sw.at[0], in_sem.at[5]).start()
    pltpu.make_async_copy(wd_hbm, sw.at[1], in_sem.at[5]).start()
    big, small = split(lf[0])
    lh[...] = big
    ll[...] = small
    far_edge(0, r, slice(0, rows))
    greet(0)
    issue(0, (0, 1))
    cross(0, (0, 1))
    others(0, r)
    issue_near(0)
    issue(0, (2,))
    cross(0, (2,))
    c_gm.wait()
    for level in range(levels):
        g = gm[level]
        fc[level] = jnp.concatenate([g[0:half], g[half:ky]], axis=1) * (
            (layers * 2 ** (level + 1)) ** -0.5
        )
    for j in range(2):
        bz6[2 * j * kz : (2 * j + 2) * kz] = bzp[0 : 2 * kz]
    bz6[4 * kz : 6 * kz] = bzp[2 * kz : 4 * kz]
    hi, lo = split(by[...].T)
    byt[...] = jnp.concatenate([hi, hi, lo], axis=1)
    drain(sw, in_sem.at[5])
    inner_image(0, range(1))
    issue(0, (3,))
    cross(0, (3,))
    inner_image(0, range(1, layers))
    exchange(0)
    back(0)
    image(0, None)
    meet(0, 0, None)
    far_edge(1, w1, spans[0])
    issue(1, (0,))
    meet(0, 1, None)
    project(1)
    a_send(1)
    far_edge(1, w1, spans[1])
    greet(1)
    issue(1, (1,))
    cross(1, (0, 1))
    others(1, w1)
    issue_near(1)
    issue(1, (2,))
    cross(1, (2,))
    add_spread(0)
    inner_image(1, range(1))
    issue(1, (3,))
    cross(1, (3,))
    inner_image(1, range(1, layers))
    early = place(dots([(r, r), (r, w1), (w1, w1)]), 0)
    exchange(1)
    back(1)
    totals = [None] * 3
    image(1, totals)
    meet(1, 0, totals)
    meet(1, 1, totals)
    late = place(totals, 3)
    flat = jnp.sum(early + late, axis=0, keepdims=True)
    gs[...] = flat
    ggat[me] = flat
    for d in range(n - 1, 0, -1):
        send(gs, ggat.at[me], out_sem, gsr, flip(me, d)).start()

    add_spread(1)
    for k in range(2):
        a_wait(k, out_sem)

        @pl.when(speaks)
        def _():
            b_wait(k, out_sem)
            b_wait(k, out_sem)

        @pl.when(jnp.logical_and(p == block - 1, z > 0))
        def _():
            low_down(k).wait_send()

        @pl.when(jnp.logical_and(p == 0, z < blocks - 1))
        def _():
            low_up(k).wait_send()

        @pl.when(me > 0)
        def _():
            drain(hs.at[k, 0], out_sem)

        @pl.when(me < n - 1)
        def _():
            drain(hs.at[k, 1], out_sem)

    drain(ggat.at[pl.ds(0, n - 1)], out_sem)
    drain(ggat.at[pl.ds(0, n - 1)], gsr)
    total = jnp.sum(ggat[...], axis=0)
    g01, g11, g02, g12, g22 = (
        jnp.broadcast_to(total[:, j : j + 1], (1, LANES)) for j in range(1, 6)
    )
    ratio = g12 / g11
    c2 = (g02 - ratio * g01) / (g22 - ratio * g12)
    c1 = g01 / g11 - ratio * c2
    coef[0] = jnp.broadcast_to(c1, (8, LANES))
    coef[1] = jnp.broadcast_to(c2, (8, LANES))


def finish(r, u1, u2, w1, w2, coef, x_hbm, res_hbm, xo, ro, x_sem, res_sem):
    layers, rows, depth = r.shape
    step, part = 8, 32
    c1 = jnp.concatenate([coef[0]] * (depth // LANES), axis=1)
    c2 = jnp.concatenate([coef[1]] * (depth // LANES), axis=1)

    def flush(buf, out, l, y, sem):
        at = pl.ds(y, part)
        pltpu.make_async_copy(buf.at[l, at], out.at[l, at], sem).start()

    for l in range(layers):
        for y in range(0, rows, step):
            a = PAD + y
            xo[l, y : y + step, :] = (
                c1 * u1[l, a : a + step, :] + c2 * u2[l, a : a + step, :]
            )
            ro[l, y : y + step, :] = (
                r[l, y : y + step, :]
                - c1 * w1[l, y : y + step, :] - c2 * w2[l, y : y + step, :]
            )
            if (y + step) % part == 0:
                flush(xo, x_hbm, l, y + step - part, x_sem)
                flush(ro, res_hbm, l, y + step - part, res_sem)
    drain(xo, x_sem)
    drain(ro, res_sem)


def on_device(right_side, sigma, wind, local_inverse, basis_y, basis_z, gamma):
    n = lax.axis_size("sub")
    block = min(8, n)
    blocks = n // block
    layers, rows, depth = right_side.shape
    ky = basis_y.shape[1]
    kz = basis_z.shape[1]
    f32, bf16 = jnp.float32, jnp.bfloat16
    packed = (ky // 2, 2 * kz)
    cube = pltpu.VMEM((layers, rows, depth), f32)
    padded = pltpu.VMEM((layers, rows + 2 * PAD, depth), f32)
    plane = pltpu.VMEM((rows, depth), f32)
    halo = pltpu.VMEM((2, 2, rows, depth), f32)
    dma = pltpu.SemaphoreType.DMA
    scratch = [
        pltpu.VMEM((2, layers, rows, depth), f32),
        pltpu.VMEM((2, rows, depth), f32),
        pltpu.VMEM((1, depth, depth), f32),
        pltpu.VMEM((ky, rows), f32),
        pltpu.VMEM((kz, depth), f32),
        pltpu.VMEM(gamma.shape, f32),
        pltpu.VMEM((depth, depth), bf16),
        pltpu.VMEM((depth, depth), bf16),
        pltpu.VMEM((2 * ky, rows), bf16),
        pltpu.VMEM((rows, 3 * ky), bf16),
        pltpu.VMEM((4 * kz, depth), bf16),
        pltpu.VMEM((6 * kz, depth), bf16),
        pltpu.VMEM((gamma.shape[0],) + packed, f32),
        pltpu.VMEM((rows + 2 * PAD, depth), f32),
        plane, plane, plane,
        pltpu.VMEM((rows, depth), bf16),
        pltpu.VMEM((rows, depth), bf16),
        halo, halo,
        pltpu.VMEM((2,) + packed, f32),
        pltpu.VMEM((2, block) + packed, f32),
        pltpu.VMEM((2,) + packed, f32),
        pltpu.VMEM((2, blocks) + packed, f32),
        pltpu.VMEM((2, 2) + packed, f32),
        pltpu.VMEM((2, 2) + packed, f32),
        pltpu.VMEM((3,) + packed, f32),
        pltpu.VMEM((1, LANES), f32),
        pltpu.VMEM((n, 1, LANES), f32),
        dma((6,)), dma,
        dma((2,)), dma((2,)), dma((2,)), dma((2, 2, 2)),
        dma,
        pltpu.SemaphoreType.REGULAR((2,)),
        pltpu.SemaphoreType.REGULAR((2,)),
    ]
    hbm = pl.BlockSpec(memory_space=pltpu.HBM)
    vmem = pl.BlockSpec(memory_space=pltpu.VMEM)
    out = jax.ShapeDtypeStruct(right_side.shape, f32)
    pieces = pl.pallas_call(
        functools.partial(kernel, n, block),
        out_shape=(cube, padded, padded, cube, cube, pltpu.VMEM((2, 8, LANES), f32)),
        in_specs=[hbm] * 7,
        out_specs=(vmem,) * 6,
        scratch_shapes=scratch,
        compiler_params=pltpu.CompilerParams(
            collective_id=0, has_side_effects=True, vmem_limit_bytes=50 * 2**20,
        ),
        name="gmres",
    )(right_side, sigma, wind, local_inverse, basis_y.T, basis_z.T, gamma)
    return pl.pallas_call(
        finish,
        out_shape=(out, out),
        in_specs=[vmem] * 6,
        out_specs=(hbm, hbm),
        scratch_shapes=[cube, cube, dma, dma],
        compiler_params=pltpu.CompilerParams(vmem_limit_bytes=24 * 2**20),
        name="finish",
    )(*pieces)


def solution(mesh):
    placed = (
        P("sub", None, None),
        P("sub", None, None),
        P("sub", None, None),
        P("sub", None, None),
        P(),
        P(),
        P(),
    )
    return jax.shard_map(
        on_device,
        mesh=mesh,
        in_specs=placed,
        out_specs=(P("sub", None, None), P("sub", None, None)),
        check_vma=False,
    )
```
